32 devices in a mesh: row: 8 (over y, x, core), col: 4 (over z).
Axes of the slice: x: 2, y: 2, z: 4, core: 2. Of those that a mesh axis runs over, the one named last changes fastest.
Arguments:
- adjacency: int32 [2560, 80], P('row', 'col'), may hold values from -2147483648 to 2147483647, as said below
- relabel: int32 [2560], P(('row', 'col')), may hold values from 0 to 2559, each once
Outputs:
- clustering: float32 [2560], P(('row', 'col'))
- transitivity: float32 [], replicated
The draws below stay inside these ranges and needn't reach their ends.
Inputs may be any that keep to these rules, and one draw needn't show every extreme that they name: The unpacked adjacency is symmetric with a zero diagonal.
All inputs are finite; a program needn't handle non-finite values.
Results may differ from the reference program's by a relative error of at most 0.0003.
Values sent between devices are 32-bit elements.
A program may use at most 128 MiB of HBM per device.

```python
import jax
import jax.numpy as jnp
from jax import lax

NV = 2560
N_ROW = 8


def draw_adjacency(key, part):
    first, second = jax.random.split(jax.random.fold_in(key, 23), 2)
    activity = jax.random.randint(first, (NV,), 1, 5)
    thresh = 1000 * activity[:, None] * activity[None, :]
    coins = jax.random.randint(second, (NV, NV), 0, 65536)
    keep = coins < thresh
    index = jnp.arange(NV)
    upper = keep & (index[None, :] > index[:, None])
    links = (upper | upper.T).astype(jnp.int32)
    bits = links.reshape(NV, NV // 32, 32)
    shifts = jnp.arange(32, dtype=jnp.int32)
    words = jnp.sum(lax.shift_left(bits, shifts[None, None, :]), axis=2)
    return words.astype(jnp.int32)


def setup_inputs(seed: int = 0) -> dict:
    key_list = jax.random.split(jax.random.key(seed), 3)
    return {
        "adjacency": draw_adjacency(jax.random.fold_in(key_list[2], 71), 0),
        "relabel": jax.random.permutation(key_list[1], NV).astype(jnp.int32),
    }


def unpack(words):
    shifts = jnp.arange(32, dtype=jnp.int32)
    bits = lax.shift_right_logical(words[:, :, None], shifts[None, None, :]) & 1
    return bits.reshape(words.shape[0], words.shape[1] * 32).astype(jnp.bfloat16)


def reference(adjacency, relabel):
    links = unpack(adjacency)
    block_rows = NV // N_ROW
    starts = jnp.arange(N_ROW, dtype=jnp.int32) * block_rows

    def one_block(offset):
        rows = lax.dynamic_slice_in_dim(links, offset.astype(jnp.int32), block_rows, 0)
        paths = jnp.dot(rows, links, preferred_element_type=jnp.float32)
        wide = rows.astype(jnp.float32)
        return jnp.sum(wide * paths, axis=1), jnp.sum(wide, axis=1)

    closed, degree = lax.map(one_block, starts)
    closed = closed.reshape(NV)
    degree = degree.reshape(NV)
    wedges = jnp.maximum(degree * (degree - 1.0), 1.0)
    ratio = closed / wedges
    clustering = jnp.take(ratio, relabel, axis=0)
    transitivity = jnp.sum(closed) / jnp.sum(wedges)
    return clustering, transitivity
```

```python
import functools

import jax
import jax.numpy as jnp
from jax import lax
from jax.experimental import pallas as pl
from jax.experimental.pallas import tpu as pltpu
from jax.sharding import PartitionSpec as P

MESH = pl.DeviceIdType.MESH
TYPE = jnp.float8_e4m3fn


def unpack(row):
    wide = jnp.broadcast_to(row, (32, row.shape[1]))
    bits = lax.shift_right_logical(wide, lax.broadcasted_iota(jnp.int32, wide.shape, 0)) & 1
    return bits.astype(jnp.float32).astype(TYPE)


def kernel(
    n_row, n_col, words_ref, relabel_ref, out_ref, total_ref,
    xs, ys, yw, x, y, hot, rel, msg, acc,
    x_send, x_recv, y_send, y_recv, m_send, m_recv, w_send, w_recv, ready, go, local_sem,
):
    n_words, n_rows = words_ref.shape
    n_all = n_row * n_col
    per = n_row // n_col
    depth = 32 * n_words
    width = msg.shape[1]
    r, c = lax.axis_index("row"), lax.axis_index("col")
    barrier = pltpu.get_barrier_semaphore()
    load_x = pltpu.make_async_copy(words_ref, xs.at[c], local_sem.at[0])
    load_y = pltpu.make_async_copy(words_ref, ys.at[r], local_sem.at[1])
    load_r = pltpu.make_async_copy(relabel_ref, rel, local_sem.at[2])
    load_x.start()
    load_y.start()
    load_r.start()
    row_peers = [lax.rem(r + o, n_row) for o in range(1, n_row)]
    last = n_row - 1
    sends_y = r >= c * per
    for p in row_peers:
        @pl.when(p >= c * per)
        def _():
            pl.semaphore_signal(barrier, inc=1, device_id=(p, c), device_id_type=MESH)

    def greet_above():
        for k in range(1, n_col):
            @pl.when(k > c)
            def _():
                pl.semaphore_signal(barrier, inc=1, device_id=(r, k), device_id_type=MESH)
    pl.when(r != last)(greet_above)
    load_x.wait()
    load_y.wait()
    pl.semaphore_wait(barrier, c + jnp.where(sends_y, n_row - 1, 0))

    def x_copy(p, to):
        return pltpu.make_async_remote_copy(
            xs.at[p], xs.at[p], x_send.at[to], x_recv.at[p], device_id=(r, to), device_id_type=MESH)

    def y_copy(p, i, to):
        return pltpu.make_async_remote_copy(
            ys.at[p], ys.at[p], y_send.at[i], y_recv.at[p], device_id=(to, c), device_id_type=MESH)

    for to in range(n_col - 1):
        @pl.when(to < c)
        def _():
            x_copy(c, to).start()

    @pl.when(sends_y)
    def _():
        for i, p in reversed(list(enumerate(row_peers))):
            y_copy(r, i, p).start()

    @pl.when(r == last)
    def _():
        greet_above()
        for k in range(n_col - 1):
            @pl.when(k < c)
            def _():
                pl.semaphore_signal(ready, inc=1, device_id=(r, k), device_id_type=MESH)

    load_r.wait()
    label = rel[...]
    owner = jnp.zeros_like(label)
    for k in range(1, n_row):
        owner += (label >= k * n_rows).astype(jnp.int32)
    place = label - owner * n_rows
    hot[...] = (lax.broadcasted_iota(jnp.int32, hot.shape, 0) == place).astype(jnp.float32).astype(jnp.bfloat16)

    def take_x(k):
        def one(w, carry):
            x[k, pl.ds(pl.multiple_of(w * 32, 32), 32), :] = unpack(xs[k, pl.ds(w, 1), :])
            return carry
        lax.fori_loop(0, n_words, one, 0, unroll=4)

    def take_y(k):
        for h in range(per):
            p = k * per + h

            @pl.when(p != r)
            def _():
                y_copy(p, 0, r).wait_recv()
        yw[...] = jnp.concatenate([ys[k * per + h] for h in range(per)], axis=1)

        def one(w, carry):
            y[k, pl.ds(pl.multiple_of(w * 32, 32), 32), :] = unpack(yw[pl.ds(w, 1), :])
            return carry
        lax.fori_loop(0, n_words, one, 0, unroll=4)

    def add(k, weight):
        paths = jnp.dot(y[k], x[k], preferred_element_type=jnp.float32)
        acc[...] += jnp.sum(paths * x[c].astype(jnp.float32), axis=0, keepdims=True) * weight

    acc[...] = jnp.zeros_like(acc)
    take_x(c)
    take_y(c)
    add(c, 1.0)

    def later_y(k, carry):
        take_y(k)
        return carry
    lax.fori_loop(c + 1, n_col, later_y, 0)

    @pl.when(r == last)
    def _():
        @pl.when(c < n_col - 1)
        def _():
            pl.semaphore_wait(ready, n_col - 1 - c)
        for p in range(n_row - 1):
            pl.semaphore_signal(go, inc=1, device_id=(p, c), device_id_type=MESH)

    def later_x(k, carry):
        x_copy(k, 0).wait_recv()
        take_x(k)
        add(k, 2.0)
        return carry
    lax.fori_loop(c + 1, n_col, later_x, 0)

    me = c * n_row + r

    @pl.when(r != last)
    def _():
        pl.semaphore_wait(go, 1)

    def padded(row):
        if width == n_rows:
            return row
        return jnp.concatenate([row, jnp.zeros((1, width - n_rows), jnp.float32)], axis=1)

    msg[pl.ds(me, 1), :] = padded(acc[...])

    def post(i, to):
        return pltpu.make_async_remote_copy(
            msg.at[pl.ds(me, 1)], msg.at[pl.ds(me, 1)], m_send.at[i], m_recv.at[me],
            device_id=(lax.rem(to, n_row), to // n_row), device_id_type=MESH)

    def post_wedges(i, to):
        mine = msg.at[pl.ds(n_all + r, 1)]
        return pltpu.make_async_remote_copy(
            mine, mine, w_send.at[i], w_recv.at[r],
            device_id=(lax.rem(to, n_row), to // n_row), device_id_type=MESH)

    others = [i + (i >= me).astype(jnp.int32) for i in range(n_all - 1)]

    @pl.when(c == 0)
    def _():
        count = jnp.zeros((n_words, n_rows), jnp.int32)
        for k in range(n_col):
            count += lax.population_count(xs[k])
        degree = jnp.sum(count, axis=0, keepdims=True).astype(jnp.float32)
        wedges = jnp.maximum(degree * (degree - 1.0), 1.0)
        msg[pl.ds(n_all + r, 1), :] = padded(wedges)
        for i, to in enumerate(others):
            post_wedges(i, to).start()

    for i, to in enumerate(others):
        post(i, to).start()

    for to in range(n_col - 1):
        @pl.when(to < c)
        def _():
            x_copy(c, to).wait_send()

    @pl.when(sends_y)
    def _():
        for i, p in enumerate(row_peers):
            y_copy(r, i, p).wait_send()

    for o in range(1, n_all):
        p = lax.rem(me + o, n_all)
        pltpu.make_async_copy(msg.at[pl.ds(p, 1)], msg.at[pl.ds(p, 1)], m_recv.at[p]).wait()
    for k in range(n_row):
        row = msg.at[pl.ds(n_all + k, 1)]

        @pl.when((c > 0) | (r != k))
        def _():
            pltpu.make_async_copy(row, row, w_recv.at[k]).wait()

    closed = msg[0:n_row, :]
    for k in range(1, n_col):
        closed += msg[k * n_row : (k + 1) * n_row, :]
    wedges = msg[n_all : n_all + n_row, :]
    inside = lax.broadcasted_iota(jnp.int32, closed.shape, 1) < n_rows
    ratio = jnp.where(inside, closed / wedges, 0.0)
    total_ref[0, 0] = jnp.sum(closed) / jnp.sum(wedges)
    high = ratio.astype(jnp.bfloat16)
    rest = ratio - high.astype(jnp.float32)
    middle = rest.astype(jnp.bfloat16)
    low = (rest - middle.astype(jnp.float32)).astype(jnp.bfloat16)
    parts = jnp.concatenate([p.astype(jnp.float32) for p in (high, middle, low)], axis=0).astype(jnp.bfloat16)
    picked = jnp.dot(parts, hot[...], preferred_element_type=jnp.float32)
    found = picked[:n_row] + picked[n_row : 2 * n_row] + picked[2 * n_row :]
    which = lax.broadcasted_iota(jnp.int32, found.shape, 0)
    out_ref[...] = jnp.sum(jnp.where(which == owner, found, 0.0), axis=0, keepdims=True)
    for i, to in enumerate(others):
        post(i, to).wait_send()

    @pl.when(c == 0)
    def _():
        for i, to in enumerate(others):
            post_wedges(i, to).wait_send()


def finish(found_ref, total_ref, out_ref, out_total_ref, sems):
    one = pltpu.make_async_copy(found_ref, out_ref, sems.at[0])
    two = pltpu.make_async_copy(total_ref, out_total_ref, sems.at[1])
    one.start()
    two.start()
    one.wait()
    two.wait()


def solution(mesh):
    n_row, n_col = mesh.shape["row"], mesh.shape["col"]
    n_all = n_row * n_col

    def body(adjacency, relabel):
        n_rows, n_words = adjacency.shape
        n_mine = relabel.shape[0]
        depth = 32 * n_words
        width = (n_rows + 127) // 128 * 128
        found, total = pl.pallas_call(
            functools.partial(kernel, n_row, n_col),
            out_shape=(pltpu.VMEM((1, n_mine), jnp.float32), pltpu.SMEM((1, 1), jnp.float32)),
            in_specs=[pl.BlockSpec(memory_space=pl.ANY)] * 2,
            out_specs=[pl.BlockSpec(memory_space=pltpu.VMEM), pl.BlockSpec(memory_space=pltpu.SMEM)],
            scratch_shapes=[
                pltpu.VMEM((n_col, n_words, n_rows), jnp.int32),
                pltpu.VMEM((n_row, n_words, n_rows), jnp.int32),
                pltpu.VMEM((n_words, depth), jnp.int32),
                pltpu.VMEM((n_col, depth, n_rows), TYPE),
                pltpu.VMEM((n_col, depth, depth), TYPE),
                pltpu.VMEM((width, n_mine), jnp.bfloat16),
                pltpu.VMEM((1, n_mine), jnp.int32),
                pltpu.VMEM((n_all + n_row, width), jnp.float32),
                pltpu.VMEM((1, n_rows), jnp.float32),
                pltpu.SemaphoreType.DMA((n_col,)),
                pltpu.SemaphoreType.DMA((n_col,)),
                pltpu.SemaphoreType.DMA((n_row - 1,)),
                pltpu.SemaphoreType.DMA((n_row,)),
                pltpu.SemaphoreType.DMA((n_all - 1,)),
                pltpu.SemaphoreType.DMA((n_all,)),
                pltpu.SemaphoreType.DMA((n_all - 1,)),
                pltpu.SemaphoreType.DMA((n_row,)),
                pltpu.SemaphoreType.REGULAR,
                pltpu.SemaphoreType.REGULAR,
                pltpu.SemaphoreType.DMA((3,)),
            ],
            compiler_params=pltpu.CompilerParams(
                collective_id=0, has_side_effects=True, vmem_limit_bytes=60000 * 1024
            ),
        )(adjacency.T, relabel.reshape(1, n_mine))
        clustering, ratio = pl.pallas_call(
            finish,
            out_shape=(
                jax.ShapeDtypeStruct((1, n_mine), jnp.float32),
                jax.ShapeDtypeStruct((1, 1), jnp.float32),
            ),
            in_specs=[pl.BlockSpec(memory_space=pltpu.VMEM), pl.BlockSpec(memory_space=pltpu.SMEM)],
            out_specs=[pl.BlockSpec(memory_space=pl.ANY)] * 2,
            scratch_shapes=[pltpu.SemaphoreType.DMA((2,))],
        )(
            pltpu.with_memory_space_constraint(found, pltpu.VMEM),
            pltpu.with_memory_space_constraint(total, pltpu.SMEM),
        )
        return clustering.reshape(n_mine), ratio.reshape(())

    placed = (P("row", "col"), P(("row", "col")))
    return jax.shard_map(
        body, mesh=mesh, in_specs=placed, out_specs=(P(("row", "col")), P()), check_vma=False
    )
```

```python
import functools

import jax
import jax.numpy as jnp
from jax import lax
from jax.experimental import pallas as pl
from jax.experimental.pallas import tpu as pltpu
from jax.sharding import PartitionSpec as P

MESH = pl.DeviceIdType.MESH
TYPE = jnp.float8_e4m3fn


def unpack(row):
    wide = jnp.broadcast_to(row, (32, row.shape[1]))
    bits = lax.shift_right_logical(wide, lax.broadcasted_iota(jnp.int32, wide.shape, 0)) & 1
    return bits.astype(jnp.int8).astype(TYPE)


def kernel(
    n_row, n_col, words_ref, relabel_ref, out_ref, total_ref,
    xs, ys, yw, x, y, mask, hot, rel, msg, bulk, acc,
    x_send, x_recv, y_send, y_recv, m_send, m_recv, ready, go, local_sem,
):
    n_words, n_rows = words_ref.shape
    n_all = n_row * n_col
    per = n_row // n_col
    depth = 32 * n_words
    width = msg.shape[2]
    r, c = lax.axis_index("row"), lax.axis_index("col")
    barrier = pltpu.get_barrier_semaphore()
    load_x = pltpu.make_async_copy(words_ref, xs.at[c], local_sem.at[0])
    load_y = pltpu.make_async_copy(words_ref, ys.at[r], local_sem.at[1])
    load_r = pltpu.make_async_copy(relabel_ref, rel, local_sem.at[2])
    load_x.start()
    load_y.start()
    load_r.start()
    row_peers = [lax.rem(r + o, n_row) for o in range(1, n_row)]
    lead = n_row - 3
    sends_y = r >= c * per
    for p in row_peers:
        @pl.when((p >= c * per) | (p == lead))
        def _():
            pl.semaphore_signal(barrier, inc=1, device_id=(p, c), device_id_type=MESH)

    def greet_above():
        for k in range(1, n_col):
            @pl.when(k > c)
            def _():
                pl.semaphore_signal(barrier, inc=1, device_id=(r, k), device_id_type=MESH)
    pl.when(r != lead)(greet_above)
    load_x.wait()
    load_y.wait()
    pl.semaphore_wait(barrier, c + jnp.where(sends_y | (r == lead), n_row - 1, 0))

    def x_copy(p, to):
        return pltpu.make_async_remote_copy(
            xs.at[p], xs.at[p], x_send.at[to], x_recv.at[p], device_id=(r, to), device_id_type=MESH)

    def y_copy(p, i, to):
        return pltpu.make_async_remote_copy(
            ys.at[p], ys.at[p], y_send.at[i], y_recv.at[p], device_id=(to, c), device_id_type=MESH)

    for to in range(n_col - 1):
        @pl.when(to < c)
        def _():
            x_copy(c, to).start()

    @pl.when(sends_y)
    def _():
        for i, p in reversed(list(enumerate(row_peers))):
            y_copy(r, i, p).start()

    @pl.when(r == lead)
    def _():
        greet_above()
        for k in range(n_col - 1):
            @pl.when(k < c)
            def _():
                pl.semaphore_signal(ready, inc=1, device_id=(r, k), device_id_type=MESH)

    load_r.wait()
    label = rel[...]
    owner = jnp.zeros_like(label)
    for k in range(1, n_row):
        owner += (label >= k * n_rows).astype(jnp.int32)
    place = label - owner * n_rows
    hot[...] = (lax.broadcasted_iota(jnp.int32, hot.shape, 0) == place).astype(jnp.float32).astype(jnp.bfloat16)

    def take_x(k):
        def one(w, carry):
            x[k, pl.ds(pl.multiple_of(w * 32, 32), 32), :] = unpack(xs[k, pl.ds(w, 1), :])
            return carry
        lax.fori_loop(0, n_words, one, 0, unroll=4)

    def take_y(k):
        for h in range(per):
            p = k * per + h

            @pl.when(p != r)
            def _():
                y_copy(p, 0, r).wait_recv()
        yw[...] = jnp.concatenate([ys[k * per + h] for h in range(per)], axis=1)

        def one(w, carry):
            y[k, pl.ds(pl.multiple_of(w * 32, 32), 32), :] = unpack(yw[pl.ds(w, 1), :])
            return carry
        lax.fori_loop(0, n_words, one, 0, unroll=4)

    def add(k, weight):
        paths = jnp.dot(y[k], x[k], preferred_element_type=jnp.float32)
        acc[...] += jnp.sum(paths * mask[...], axis=0, keepdims=True) * weight

    def wait_x(k):
        x_copy(k, 0).wait_recv()
        take_x(k)

    def hear_and_tell():
        @pl.when(c < n_col - 1)
        def _():
            pl.semaphore_wait(ready, n_col - 1 - c)
        for p in row_peers:
            pl.semaphore_signal(go, inc=1, device_id=(p, c), device_id_type=MESH)

    acc[...] = jnp.zeros_like(acc)
    take_x(c)
    mask[...] = x[c].astype(jnp.float32)
    for j in range(n_col):
        if j == n_col - 1:
            pl.when(r == lead)(hear_and_tell)
            pl.when(c < n_col - 1)(lambda: wait_x(c + 1))
        own = r // per
        k = own ^ j if n_col & (n_col - 1) == 0 else lax.rem(own + j, n_col)
        pl.when(k >= c)(lambda: take_y(k))
        pl.when(k == c)(lambda: add(c, 1.0))
    pl.when(c < n_col - 1)(lambda: add(c + 1, 2.0))

    def later_x(k, carry):
        wait_x(k)
        add(k, 2.0)
        return carry
    lax.fori_loop(c + 2, n_col, later_x, 0)

    me = c * n_row + r

    @pl.when(r != lead)
    def _():
        pl.semaphore_wait(go, 1)

    def padded(row):
        if width == n_rows:
            return row
        return jnp.concatenate([row, jnp.zeros((1, width - n_rows), jnp.float32)], axis=1)

    def post(planes, to):
        mine = msg.at[planes, pl.ds(r, 1), :]
        return pltpu.make_async_remote_copy(
            mine, mine, m_send, m_recv, device_id=(lax.rem(to, n_row), to // n_row), device_id_type=MESH)

    others = [i + (i >= me).astype(jnp.int32) for i in range(n_all - 1)]

    @pl.when(c == 0)
    def _():
        count = jnp.zeros((n_words, n_rows), jnp.int32)
        for k in range(n_col):
            count += lax.population_count(xs[k])
        degree = jnp.sum(count, axis=0, keepdims=True).astype(jnp.float32)
        msg[0, pl.ds(r, 1), :] = padded(acc[...])
        msg[1, pl.ds(r, 1), :] = padded(jnp.maximum(degree * (degree - 1.0), 1.0))
        for to in others:
            post(pl.ds(0, 2), to).start()

    @pl.when(c > 0)
    def _():
        msg[c + 1, pl.ds(r, 1), :] = padded(acc[...])
        for to in others:
            post(pl.ds(c + 1, 1), to).start()

    for to in range(n_col - 1):
        @pl.when(to < c)
        def _():
            x_copy(c, to).wait_send()

    @pl.when(sends_y)
    def _():
        for i, p in enumerate(row_peers):
            y_copy(r, i, p).wait_send()

    def take(rows, sem):
        pltpu.make_async_copy(bulk.at[pl.ds(0, rows)], bulk.at[pl.ds(0, rows)], sem).wait()
    pl.when(c == 0)(lambda: take(n_all - 1 + n_row - 1, m_recv))
    pl.when(c > 0)(lambda: take(n_all - 1 + n_row, m_recv))

    closed = msg[0]
    for k in range(1, n_col):
        closed += msg[k + 1]
    wedges = msg[1]
    inside = lax.broadcasted_iota(jnp.int32, closed.shape, 1) < n_rows
    ratio = jnp.where(inside, closed / wedges, 0.0)
    def whole(part):
        return jnp.sum(jnp.sum(part, axis=0, keepdims=True), axis=1, keepdims=True)
    total = whole(closed) / whole(wedges)
    total_ref[0, 0] = total[0, 0]
    high = ratio.astype(jnp.bfloat16)
    rest = ratio - high.astype(jnp.float32)
    middle = rest.astype(jnp.bfloat16)
    low = (rest - middle.astype(jnp.float32)).astype(jnp.bfloat16)
    parts = jnp.concatenate([p.astype(jnp.float32) for p in (high, middle, low)], axis=0).astype(jnp.bfloat16)
    picked = jnp.dot(parts, hot[...], preferred_element_type=jnp.float32)
    found = picked[:n_row] + picked[n_row : 2 * n_row] + picked[2 * n_row :]
    which = lax.broadcasted_iota(jnp.int32, found.shape, 0)
    out_ref[...] = jnp.sum(jnp.where(which == owner, found, 0.0), axis=0, keepdims=True)
    pl.when(c == 0)(lambda: take(2 * (n_all - 1), m_send))
    pl.when(c > 0)(lambda: take(n_all - 1, m_send))


def finish(found_ref, total_ref, out_ref, out_total_ref, sems):
    one = pltpu.make_async_copy(found_ref, out_ref, sems.at[0])
    two = pltpu.make_async_copy(total_ref, out_total_ref, sems.at[1])
    one.start()
    two.start()
    one.wait()
    two.wait()


def solution(mesh):
    n_row, n_col = mesh.shape["row"], mesh.shape["col"]
    n_all = n_row * n_col

    def body(adjacency, relabel):
        n_rows, n_words = adjacency.shape
        n_mine = relabel.shape[0]
        depth = 32 * n_words
        width = (n_rows + 127) // 128 * 128
        found, total = pl.pallas_call(
            functools.partial(kernel, n_row, n_col),
            out_shape=(pltpu.VMEM((1, n_mine), jnp.float32), pltpu.SMEM((1, 1), jnp.float32)),
            in_specs=[pl.BlockSpec(memory_space=pl.ANY)] * 2,
            out_specs=[pl.BlockSpec(memory_space=pltpu.VMEM), pl.BlockSpec(memory_space=pltpu.SMEM)],
            scratch_shapes=[
                pltpu.VMEM((n_col, n_words, n_rows), jnp.int32),
                pltpu.VMEM((n_row, n_words, n_rows), jnp.int32),
                pltpu.VMEM((n_words, depth), jnp.int32),
                pltpu.VMEM((n_col, depth, n_rows), TYPE),
                pltpu.VMEM((n_col, depth, depth), TYPE),
                pltpu.VMEM((depth, n_rows), jnp.float32),
                pltpu.VMEM((width, n_mine), jnp.bfloat16),
                pltpu.VMEM((1, n_mine), jnp.int32),
                pltpu.VMEM((n_col + 1, n_row, width), jnp.float32),
                pltpu.VMEM((2 * n_all, 1, width), jnp.float32),
                pltpu.VMEM((1, n_rows), jnp.float32),
                pltpu.SemaphoreType.DMA((n_col,)),
                pltpu.SemaphoreType.DMA((n_col,)),
                pltpu.SemaphoreType.DMA((n_row - 1,)),
                pltpu.SemaphoreType.DMA((n_row,)),
                pltpu.SemaphoreType.DMA,
                pltpu.SemaphoreType.DMA,
                pltpu.SemaphoreType.REGULAR,
                pltpu.SemaphoreType.REGULAR,
                pltpu.SemaphoreType.DMA((3,)),
            ],
            compiler_params=pltpu.CompilerParams(
                collective_id=0, has_side_effects=True, vmem_limit_bytes=60000 * 1024
            ),
        )(adjacency.T, relabel.reshape(1, n_mine))
        clustering, ratio = pl.pallas_call(
            finish,
            out_shape=(
                jax.ShapeDtypeStruct((1, n_mine), jnp.float32),
                jax.ShapeDtypeStruct((1, 1), jnp.float32),
            ),
            in_specs=[pl.BlockSpec(memory_space=pltpu.VMEM), pl.BlockSpec(memory_space=pltpu.SMEM)],
            out_specs=[pl.BlockSpec(memory_space=pl.ANY)] * 2,
            scratch_shapes=[pltpu.SemaphoreType.DMA((2,))],
        )(
            pltpu.with_memory_space_constraint(found, pltpu.VMEM),
            pltpu.with_memory_space_constraint(total, pltpu.SMEM),
        )
        return clustering.reshape(n_mine), ratio.reshape(())

    placed = (P("row", "col"), P(("row", "col")))
    return jax.shard_map(
        body, mesh=mesh, in_specs=placed, out_specs=(P(("row", "col")), P()), check_vma=False
    )
```

```python
import functools

import jax
import jax.numpy as jnp
from jax import lax
from jax.experimental import pallas as pl
from jax.experimental.pallas import tpu as pltpu
from jax.sharding import PartitionSpec as P

MESH = pl.DeviceIdType.MESH
TYPE = jnp.float8_e4m3fn


def unpack(row):
    wide = jnp.broadcast_to(row, (32, row.shape[1]))
    bits = lax.shift_right_logical(wide, lax.broadcasted_iota(jnp.int32, wide.shape, 0)) & 1
    return bits.astype(jnp.int8).astype(TYPE)


def kernel(
    n_row, n_col, words_ref, relabel_ref, out_ref, total_ref,
    raw, px, py, tails, x, y, mask, hot, rel, msg, bulk, acc,
    x_send, x_recv, y_send, y_recv, m_send, m_recv, ready, go, local_sem,
):
    n_words, n_rows = words_ref.shape
    n_all = n_row * n_col
    per = n_row // n_col
    depth = 32 * n_words
    width = msg.shape[2]
    r, c = lax.axis_index("row"), lax.axis_index("col")
    barrier = pltpu.get_barrier_semaphore()
    load = pltpu.make_async_copy(words_ref, raw, local_sem.at[0])
    load_r = pltpu.make_async_copy(relabel_ref, rel, local_sem.at[1])
    load.start()
    load_r.start()
    full, half = n_rows // 128, n_rows % 128
    packed = full * n_words
    if half:
        assert half == 64 and n_words % 2 == 0 and per == 2
    if n_row & (n_row - 1) == 0:
        row_peers = [r ^ o for o in range(1, n_row)]
    else:
        row_peers = [lax.rem(r + o, n_row) for o in range(1, n_row)]
    lead = n_row - 3
    sends_y = r >= c * per
    for p in row_peers:
        @pl.when((p >= c * per) | (p == lead))
        def _():
            pl.semaphore_signal(barrier, inc=1, device_id=(p, c), device_id_type=MESH)

    def greet_above():
        for k in range(1, n_col):
            @pl.when(k > c)
            def _():
                pl.semaphore_signal(barrier, inc=1, device_id=(r, k), device_id_type=MESH)
    pl.when(r != lead)(greet_above)
    load.wait()
    for f in range(full):
        chunk = raw[:, f * 128 : (f + 1) * 128]
        px[c, f * n_words : (f + 1) * n_words, :] = chunk
        py[r, f * n_words : (f + 1) * n_words, :] = chunk
    if half:
        ends = raw[:, full * 128 :]
        ends = jnp.concatenate([ends[: n_words // 2], ends[n_words // 2 :]], axis=1)
        ends = jnp.concatenate([ends, jnp.zeros((px.shape[1] - packed - n_words // 2, 128), jnp.int32)], axis=0)
        px[c, packed:, :] = ends
        py[r, packed:, :] = ends
    pl.semaphore_wait(barrier, c + jnp.where(sends_y | (r == lead), n_row - 1, 0))

    def x_copy(p, to):
        return pltpu.make_async_remote_copy(
            px.at[p], px.at[p], x_send.at[to], x_recv.at[p], device_id=(r, to), device_id_type=MESH)

    def y_copy(p, i, to):
        return pltpu.make_async_remote_copy(
            py.at[p], py.at[p], y_send.at[i], y_recv.at[p], device_id=(to, c), device_id_type=MESH)

    for to in range(n_col - 1):
        @pl.when(to < c)
        def _():
            x_copy(c, to).start()

    @pl.when(sends_y)
    def _():
        for i, p in reversed(list(enumerate(row_peers))):
            y_copy(r, i, p).start()

    @pl.when(r == lead)
    def _():
        greet_above()
        for k in range(n_col - 1):
            @pl.when(k < c)
            def _():
                pl.semaphore_signal(ready, inc=1, device_id=(r, k), device_id_type=MESH)

    load_r.wait()
    label = rel[...]
    owner = jnp.zeros_like(label)
    for k in range(1, n_row):
        owner += (label >= k * n_rows).astype(jnp.int32)
    place = label - owner * n_rows
    hot[...] = (lax.broadcasted_iota(jnp.int32, hot.shape, 0) == place).astype(jnp.float32).astype(jnp.bfloat16)

    def place_of(w):
        if not half:
            return w
        q = lax.rem(w, n_rows // 32)
        b = w // (n_rows // 32)
        return jnp.where(q < 4 * full, b * 4 * full + q, per * 4 * full + 2 * b + q - 4 * full)

    def at(w):
        return pl.ds(pl.multiple_of(place_of(w) * 32, 32), 32)

    def take_x(k):
        if half:
            def pair(w, carry):
                both = (at(w), at(w + n_words // 2))
                for h in range(2):
                    for f in range(full):
                        row = px[k, pl.ds(f * n_words + h * (n_words // 2) + w, 1), :]
                        x[k, both[h], f * 128 : (f + 1) * 128] = unpack(row)
                ends = unpack(px[k, pl.ds(packed + w, 1), :])
                for h in range(2):
                    x[k, both[h], full * 128 :] = ends[:, h * 64 : (h + 1) * 64]
                return carry
            lax.fori_loop(0, n_words // 2, pair, 0, unroll=2)
        else:
            def one(w, carry):
                for f in range(full):
                    x[k, at(w), f * 128 : (f + 1) * 128] = unpack(px[k, pl.ds(f * n_words + w, 1), :])
                return carry
            lax.fori_loop(0, n_words, one, 0, unroll=4)

    def take_y(k):
        for h in range(per):
            p = k * per + h

            @pl.when(p != r)
            def _():
                y_copy(p, 0, r).wait_recv()
        if half:
            a = py[k * per, packed : packed + n_words // 2, :]
            b = py[k * per + 1, packed : packed + n_words // 2, :]
            left = lax.broadcasted_iota(jnp.int32, a.shape, 1) < 64
            tails[0] = jnp.where(left, a, pltpu.roll(b, 64, 1))
            tails[1] = jnp.where(left, pltpu.roll(a, 64, 1), b)

        def one(w, carry):
            for h in range(per):
                for f in range(full):
                    row = py[k * per + h, pl.ds(f * n_words + w, 1), :]
                    y[k, at(w), (h * full + f) * 128 : (h * full + f + 1) * 128] = unpack(row)
            if half:
                row = tails[w // (n_words // 2), pl.ds(lax.rem(w, n_words // 2), 1), :]
                y[k, at(w), per * full * 128 :] = unpack(row)
            return carry
        lax.fori_loop(0, n_words, one, 0, unroll=4)

    def add(k):
        paths = jnp.dot(y[k], x[k], preferred_element_type=jnp.float32)
        acc[...] += jnp.sum(paths * mask[...], axis=0, keepdims=True) * jnp.where(k == c, 1.0, 2.0)

    def wait_x(k):
        x_copy(k, 0).wait_recv()
        take_x(k)

    def hear_and_tell():
        @pl.when(c < n_col - 1)
        def _():
            pl.semaphore_wait(ready, n_col - 1 - c)
        for p in row_peers:
            pl.semaphore_signal(go, inc=1, device_id=(p, c), device_id_type=MESH)

    acc[...] = jnp.zeros_like(acc)
    take_x(c)
    mask[...] = x[c].astype(jnp.float32)
    own = r // per
    twos = n_col & (n_col - 1) == 0

    def step(j, carry):
        pl.when((j == n_col - 2) & (r == lead))(hear_and_tell)
        k = own ^ j if twos else lax.rem(own + j, n_col)

        @pl.when(k >= c)
        def _():
            take_y(k)
            pl.when((k == c) | (k < c + j))(lambda: add(k))
        up = c + j

        @pl.when((j > 0) & (up < n_col))
        def _():
            wait_x(up)
            turn = up ^ own if twos else lax.rem(up + n_col - own, n_col)
            pl.when(turn <= j)(lambda: add(up))
        return carry
    lax.fori_loop(0, n_col, step, 0)

    me = c * n_row + r

    @pl.when(r != lead)
    def _():
        pl.semaphore_wait(go, 1)

    def padded(row):
        if width == n_rows:
            return row
        return jnp.concatenate([row, jnp.zeros((1, width - n_rows), jnp.float32)], axis=1)

    def post(planes, to):
        mine = msg.at[planes, pl.ds(r, 1), :]
        return pltpu.make_async_remote_copy(
            mine, mine, m_send, m_recv, device_id=(lax.rem(to, n_row), to // n_row), device_id_type=MESH)

    others = [i + (i >= me).astype(jnp.int32) for i in range(n_all - 1)]

    @pl.when(c == 0)
    def _():
        count = jnp.zeros(px.shape[1:], jnp.int32)
        for k in range(n_col):
            count += lax.population_count(px[k])
        parts = [jnp.sum(count[f * n_words : (f + 1) * n_words], axis=0, keepdims=True) for f in range(full)]
        if half:
            ends = jnp.sum(count[packed : packed + n_words // 2], axis=0, keepdims=True)
            parts.append(ends + pltpu.roll(ends, 64, 1))
        degree = jnp.concatenate(parts, axis=1).astype(jnp.float32)
        wedges = jnp.maximum(degree * (degree - 1.0), 1.0)
        msg[0, pl.ds(r, 1), :] = padded(acc[...])
        msg[1, pl.ds(r, 1), :] = jnp.where(lax.broadcasted_iota(jnp.int32, wedges.shape, 1) < n_rows, wedges, 0.0)
        for to in others:
            post(pl.ds(0, 2), to).start()

    @pl.when(c > 0)
    def _():
        msg[c + 1, pl.ds(r, 1), :] = padded(acc[...])
        for to in others:
            post(pl.ds(c + 1, 1), to).start()

    for to in range(n_col - 1):
        @pl.when(to < c)
        def _():
            x_copy(c, to).wait_send()

    @pl.when(sends_y)
    def _():
        for i, p in enumerate(row_peers):
            y_copy(r, i, p).wait_send()

    def take(rows, sem):
        pltpu.make_async_copy(bulk.at[pl.ds(0, rows)], bulk.at[pl.ds(0, rows)], sem).wait()
    pl.when(c == 0)(lambda: take(n_all - 1 + n_row - 1, m_recv))
    pl.when(c > 0)(lambda: take(n_all - 1 + n_row, m_recv))

    closed = msg[0]
    for k in range(1, n_col):
        closed += msg[k + 1]
    wedges = msg[1]
    inside = lax.broadcasted_iota(jnp.int32, closed.shape, 1) < n_rows
    ratio = jnp.where(inside, closed / wedges, 0.0)
    def whole(part):
        return jnp.sum(jnp.sum(part, axis=0, keepdims=True), axis=1, keepdims=True)
    total = whole(closed) / whole(wedges)
    total_ref[0, 0] = total[0, 0]
    high = ratio.astype(jnp.bfloat16)
    rest = ratio - high.astype(jnp.float32)
    middle = rest.astype(jnp.bfloat16)
    low = (rest - middle.astype(jnp.float32)).astype(jnp.bfloat16)
    parts = jnp.concatenate([p.astype(jnp.float32) for p in (high, middle, low)], axis=0).astype(jnp.bfloat16)
    picked = jnp.dot(parts, hot[...], preferred_element_type=jnp.float32)
    found = picked[:n_row] + picked[n_row : 2 * n_row] + picked[2 * n_row :]
    which = lax.broadcasted_iota(jnp.int32, found.shape, 0)
    out_ref[...] = jnp.sum(jnp.where(which == owner, found, 0.0), axis=0, keepdims=True)
    pl.when(c == 0)(lambda: take(2 * (n_all - 1), m_send))
    pl.when(c > 0)(lambda: take(n_all - 1, m_send))


def finish(found_ref, total_ref, out_ref, out_total_ref, sems):
    one = pltpu.make_async_copy(found_ref, out_ref, sems.at[0])
    two = pltpu.make_async_copy(total_ref, out_total_ref, sems.at[1])
    one.start()
    two.start()
    one.wait()
    two.wait()


def solution(mesh):
    n_row, n_col = mesh.shape["row"], mesh.shape["col"]
    n_all = n_row * n_col

    def body(adjacency, relabel):
        n_rows, n_words = adjacency.shape
        n_mine = relabel.shape[0]
        depth = 32 * n_words
        width = (n_rows + 127) // 128 * 128
        lines = (n_rows * n_words // 128 + 7) // 8 * 8
        found, total = pl.pallas_call(
            functools.partial(kernel, n_row, n_col),
            out_shape=(pltpu.VMEM((1, n_mine), jnp.float32), pltpu.SMEM((1, 1), jnp.float32)),
            in_specs=[pl.BlockSpec(memory_space=pl.ANY)] * 2,
            out_specs=[pl.BlockSpec(memory_space=pltpu.VMEM), pl.BlockSpec(memory_space=pltpu.SMEM)],
            scratch_shapes=[
                pltpu.VMEM((n_words, n_rows), jnp.int32),
                pltpu.VMEM((n_col, lines, 128), jnp.int32),
                pltpu.VMEM((n_row, lines, 128), jnp.int32),
                pltpu.VMEM((2, n_words // 2, 128), jnp.int32),
                pltpu.VMEM((n_col, depth, n_rows), TYPE),
                pltpu.VMEM((n_col, depth, depth), TYPE),
                pltpu.VMEM((depth, n_rows), jnp.float32),
                pltpu.VMEM((width, n_mine), jnp.bfloat16),
                pltpu.VMEM((1, n_mine), jnp.int32),
                pltpu.VMEM((n_col + 1, n_row, width), jnp.float32),
                pltpu.VMEM((2 * n_all, 1, width), jnp.float32),
                pltpu.VMEM((1, n_rows), jnp.float32),
                pltpu.SemaphoreType.DMA((n_col,)),
                pltpu.SemaphoreType.DMA((n_col,)),
                pltpu.SemaphoreType.DMA((n_row - 1,)),
                pltpu.SemaphoreType.DMA((n_row,)),
                pltpu.SemaphoreType.DMA,
                pltpu.SemaphoreType.DMA,
                pltpu.SemaphoreType.REGULAR,
                pltpu.SemaphoreType.REGULAR,
                pltpu.SemaphoreType.DMA((2,)),
            ],
            compiler_params=pltpu.CompilerParams(
                collective_id=0, has_side_effects=True, vmem_limit_bytes=60000 * 1024
            ),
        )(adjacency.T, relabel.reshape(1, n_mine))
        clustering, ratio = pl.pallas_call(
            finish,
            out_shape=(
                jax.ShapeDtypeStruct((1, n_mine), jnp.float32),
                jax.ShapeDtypeStruct((1, 1), jnp.float32),
            ),
            in_specs=[pl.BlockSpec(memory_space=pltpu.VMEM), pl.BlockSpec(memory_space=pltpu.SMEM)],
            out_specs=[pl.BlockSpec(memory_space=pl.ANY)] * 2,
            scratch_shapes=[pltpu.SemaphoreType.DMA((2,))],
        )(
            pltpu.with_memory_space_constraint(found, pltpu.VMEM),
            pltpu.with_memory_space_constraint(total, pltpu.SMEM),
        )
        return clustering.reshape(n_mine), ratio.reshape(())

    placed = (P("row", "col"), P(("row", "col")))
    return jax.shard_map(
        body, mesh=mesh, in_specs=placed, out_specs=(P(("row", "col")), P()), check_vma=False
    )
```

```python
import functools

import jax
import jax.numpy as jnp
from jax import lax
from jax.experimental import pallas as pl
from jax.experimental.pallas import tpu as pltpu
from jax.sharding import PartitionSpec as P

MESH = pl.DeviceIdType.MESH
TYPE = jnp.float8_e4m3fn


def unpack(row):
    wide = jnp.broadcast_to(row, (32, row.shape[1]))
    bits = lax.shift_right_logical(wide, lax.broadcasted_iota(jnp.int32, wide.shape, 0)) & 1
    return bits.astype(jnp.int8).astype(TYPE)


def kernel(
    n_row, n_col, words_ref, relabel_ref, out_ref, total_ref,
    raw, px, py, tails, x, y, mask, hot, rel, msg, bulk, acc,
    x_send, x_recv, y_send, y_recv, m_send, m_recv, ready, go, local_sem,
):
    n_words, n_rows = words_ref.shape
    n_all = n_row * n_col
    per = n_row // n_col
    depth = 32 * n_words
    width = msg.shape[2]
    r, c = lax.axis_index("row"), lax.axis_index("col")
    barrier = pltpu.get_barrier_semaphore()
    load = pltpu.make_async_copy(words_ref, raw, local_sem.at[0])
    load_r = pltpu.make_async_copy(relabel_ref, rel, local_sem.at[1])
    load.start()
    load_r.start()
    full, half = n_rows // 128, n_rows % 128
    packed = full * n_words
    if half:
        assert half == 64 and n_words % 2 == 0 and per == 2
    if n_row & (n_row - 1) == 0:
        row_peers = [r ^ o for o in range(1, n_row)]
    else:
        row_peers = [lax.rem(r + o, n_row) for o in range(1, n_row)]
    lead = n_row - 3
    sends_y = r >= c * per
    for p in row_peers:
        @pl.when((p >= c * per) | (p == lead))
        def _():
            pl.semaphore_signal(barrier, inc=1, device_id=(p, c), device_id_type=MESH)

    def greet_above():
        for k in range(1, n_col):
            @pl.when(k > c)
            def _():
                pl.semaphore_signal(barrier, inc=1, device_id=(r, k), device_id_type=MESH)
    pl.when(r != lead)(greet_above)
    load.wait()
    for f in range(full):
        chunk = raw[:, f * 128 : (f + 1) * 128]
        px[c, f * n_words : (f + 1) * n_words, :] = chunk
        py[r, f * n_words : (f + 1) * n_words, :] = chunk
    if half:
        ends = raw[:, full * 128 :]
        ends = jnp.concatenate([ends[: n_words // 2], ends[n_words // 2 :]], axis=1)
        ends = jnp.concatenate([ends, jnp.zeros((px.shape[1] - packed - n_words // 2, 128), jnp.int32)], axis=0)
        px[c, packed:, :] = ends
        py[r, packed:, :] = ends
    pl.semaphore_wait(barrier, c + jnp.where(sends_y | (r == lead), n_row - 1, 0))

    def x_copy(p, to):
        return pltpu.make_async_remote_copy(
            px.at[p], px.at[p], x_send.at[to], x_recv.at[p], device_id=(r, to), device_id_type=MESH)

    def y_copy(p, i, to):
        return pltpu.make_async_remote_copy(
            py.at[p], py.at[p], y_send.at[i], y_recv.at[p], device_id=(to, c), device_id_type=MESH)

    for to in range(n_col - 1):
        @pl.when(to < c)
        def _():
            x_copy(c, to).start()

    @pl.when(sends_y)
    def _():
        for i, p in reversed(list(enumerate(row_peers))):
            y_copy(r, i, p).start()

    @pl.when(r == lead)
    def _():
        greet_above()
        for k in range(n_col - 1):
            @pl.when(k < c)
            def _():
                pl.semaphore_signal(ready, inc=1, device_id=(r, k), device_id_type=MESH)

    load_r.wait()
    label = rel[...]
    owner = jnp.zeros_like(label)
    for k in range(1, n_row):
        owner += (label >= k * n_rows).astype(jnp.int32)
    place = label - owner * n_rows
    hot[...] = (lax.broadcasted_iota(jnp.int32, hot.shape, 0) == place).astype(jnp.float32).astype(jnp.bfloat16)

    def at(w):
        b, q = divmod(w, n_rows // 32)
        if half:
            w = b * 4 * full + q if q < 4 * full else per * 4 * full + 2 * b + q - 4 * full
        return slice(w * 32, w * 32 + 32)

    def take_x(k):
        if half:
            ends = px[k, packed : packed + n_words // 2, :]
            tails[0] = ends
            tails[1] = pltpu.roll(ends, 64, 1)
        for w in range(n_words):
            for f in range(full):
                x[k, at(w), f * 128 : (f + 1) * 128] = unpack(px[k, f * n_words + w : f * n_words + w + 1, :])
            if half:
                h, q = divmod(w, n_words // 2)
                x[k, at(w), full * 128 :] = unpack(tails[h, q : q + 1, :])

    def take_y(k):
        for h in range(per):
            p = k * per + h

            @pl.when(p != r)
            def _():
                y_copy(p, 0, r).wait_recv()
        if half:
            a = py[k * per, packed : packed + n_words // 2, :]
            b = py[k * per + 1, packed : packed + n_words // 2, :]
            left = lax.broadcasted_iota(jnp.int32, a.shape, 1) < 64
            tails[0] = jnp.where(left, a, pltpu.roll(b, 64, 1))
            tails[1] = jnp.where(left, pltpu.roll(a, 64, 1), b)
        for w in range(n_words):
            for h in range(per):
                for f in range(full):
                    row = py[k * per + h, f * n_words + w : f * n_words + w + 1, :]
                    y[k, at(w), (h * full + f) * 128 : (h * full + f + 1) * 128] = unpack(row)
            if half:
                h, q = divmod(w, n_words // 2)
                y[k, at(w), per * full * 128 :] = unpack(tails[h, q : q + 1, :])

    def add(k):
        paths = jnp.dot(y[k], x[k], preferred_element_type=jnp.float32)
        acc[...] += jnp.sum(paths * mask[...], axis=0, keepdims=True) * jnp.where(k == c, 1.0, 2.0)

    def wait_x(k):
        x_copy(k, 0).wait_recv()
        take_x(k)

    def hear_and_tell():
        @pl.when(c < n_col - 1)
        def _():
            pl.semaphore_wait(ready, n_col - 1 - c)
        for p in row_peers:
            pl.semaphore_signal(go, inc=1, device_id=(p, c), device_id_type=MESH)

    pl.when((r == lead) & (c == n_col - 1))(hear_and_tell)
    acc[...] = jnp.zeros_like(acc)
    take_x(c)
    mask[...] = x[c].astype(jnp.float32)
    own = r // per

    def step(j, carry):
        k = jnp.where(j == 0, own, n_col - j - (own >= n_col - j).astype(jnp.int32))

        @pl.when(k >= c)
        def _():
            take_y(k)
            pl.when((k == c) | (k < c + j))(lambda: add(k))
        pl.when((j == 1) & (r == lead) & (c < n_col - 1))(hear_and_tell)
        up = c + j
        turn = jnp.where(up == own, 0, n_col - up - (up < own).astype(jnp.int32))

        @pl.when((j > 0) & (up < n_col))
        def _():
            wait_x(up)
            pl.when(turn <= j)(lambda: add(up))
        return carry
    lax.fori_loop(0, n_col, step, 0)

    me = c * n_row + r

    @pl.when(r != lead)
    def _():
        pl.semaphore_wait(go, 1)

    def inner(row):
        return jnp.where(lax.broadcasted_iota(jnp.int32, row.shape, 1) < n_rows, row, 0.0)

    def post(planes, to):
        mine = msg.at[planes, pl.ds(r, 1), :]
        return pltpu.make_async_remote_copy(
            mine, mine, m_send, m_recv, device_id=(lax.rem(to, n_row), to // n_row), device_id_type=MESH)

    others = [i + (i >= me).astype(jnp.int32) for i in range(n_all - 1)]

    @pl.when(c == 0)
    def _():
        count = jnp.zeros(px.shape[1:], jnp.int32)
        for k in range(n_col):
            count += lax.population_count(px[k])
        parts = [jnp.sum(count[f * n_words : (f + 1) * n_words], axis=0, keepdims=True) for f in range(full)]
        if half:
            ends = jnp.sum(count[packed : packed + n_words // 2], axis=0, keepdims=True)
            parts.append(ends + pltpu.roll(ends, 64, 1))
        degree = jnp.concatenate(parts, axis=1).astype(jnp.float32)
        wedges = jnp.maximum(degree * (degree - 1.0), 1.0)
        msg[0, pl.ds(r, 1), :] = inner(acc[...])
        msg[1, pl.ds(r, 1), :] = inner(wedges)
        for to in others:
            post(pl.ds(0, 2), to).start()

    @pl.when(c > 0)
    def _():
        msg[c + 1, pl.ds(r, 1), :] = inner(acc[...])
        for to in others:
            post(pl.ds(c + 1, 1), to).start()

    for to in range(n_col - 1):
        @pl.when(to < c)
        def _():
            x_copy(c, to).wait_send()

    @pl.when(sends_y)
    def _():
        for i, p in enumerate(row_peers):
            y_copy(r, i, p).wait_send()

    def take(rows, sem):
        pltpu.make_async_copy(bulk.at[pl.ds(0, rows)], bulk.at[pl.ds(0, rows)], sem).wait()
    pl.when(c == 0)(lambda: take(n_all - 1 + n_row - 1, m_recv))
    pl.when(c > 0)(lambda: take(n_all - 1 + n_row, m_recv))

    closed = msg[0]
    for k in range(1, n_col):
        closed += msg[k + 1]
    wedges = msg[1]
    inside = lax.broadcasted_iota(jnp.int32, closed.shape, 1) < n_rows
    ratio = jnp.where(inside, closed / wedges, 0.0)
    def whole(part):
        return jnp.sum(jnp.sum(part, axis=0, keepdims=True), axis=1, keepdims=True)
    total = whole(closed) / whole(wedges)
    total_ref[0, 0] = total[0, 0]
    high = ratio.astype(jnp.bfloat16)
    rest = ratio - high.astype(jnp.float32)
    middle = rest.astype(jnp.bfloat16)
    low = (rest - middle.astype(jnp.float32)).astype(jnp.bfloat16)
    parts = jnp.concatenate([p.astype(jnp.float32) for p in (high, middle, low)], axis=0).astype(jnp.bfloat16)
    picked = jnp.dot(parts, hot[...], preferred_element_type=jnp.float32)
    found = picked[:n_row] + picked[n_row : 2 * n_row] + picked[2 * n_row :]
    which = lax.broadcasted_iota(jnp.int32, found.shape, 0)
    out_ref[...] = jnp.sum(jnp.where(which == owner, found, 0.0), axis=0, keepdims=True)
    pl.when(c == 0)(lambda: take(2 * (n_all - 1), m_send))
    pl.when(c > 0)(lambda: take(n_all - 1, m_send))


def finish(found_ref, total_ref, out_ref, out_total_ref, sems):
    one = pltpu.make_async_copy(found_ref, out_ref, sems.at[0])
    two = pltpu.make_async_copy(total_ref, out_total_ref, sems.at[1])
    one.start()
    two.start()
    one.wait()
    two.wait()


def solution(mesh):
    n_row, n_col = mesh.shape["row"], mesh.shape["col"]
    n_all = n_row * n_col

    def body(adjacency, relabel):
        n_rows, n_words = adjacency.shape
        n_mine = relabel.shape[0]
        depth = 32 * n_words
        width = (n_rows + 127) // 128 * 128
        lines = (n_rows * n_words // 128 + 7) // 8 * 8
        found, total = pl.pallas_call(
            functools.partial(kernel, n_row, n_col),
            out_shape=(pltpu.VMEM((1, n_mine), jnp.float32), pltpu.SMEM((1, 1), jnp.float32)),
            in_specs=[pl.BlockSpec(memory_space=pl.ANY)] * 2,
            out_specs=[pl.BlockSpec(memory_space=pltpu.VMEM), pl.BlockSpec(memory_space=pltpu.SMEM)],
            scratch_shapes=[
                pltpu.VMEM((n_words, n_rows), jnp.int32),
                pltpu.VMEM((n_col, lines, 128), jnp.int32),
                pltpu.VMEM((n_row, lines, 128), jnp.int32),
                pltpu.VMEM((2, n_words // 2, 128), jnp.int32),
                pltpu.VMEM((n_col, depth, width), TYPE),
                pltpu.VMEM((n_col, depth, depth), TYPE),
                pltpu.VMEM((depth, width), jnp.float32),
                pltpu.VMEM((width, n_mine), jnp.bfloat16),
                pltpu.VMEM((1, n_mine), jnp.int32),
                pltpu.VMEM((n_col + 1, n_row, width), jnp.float32),
                pltpu.VMEM((2 * n_all, 1, width), jnp.float32),
                pltpu.VMEM((1, width), jnp.float32),
                pltpu.SemaphoreType.DMA((n_col,)),
                pltpu.SemaphoreType.DMA((n_col,)),
                pltpu.SemaphoreType.DMA((n_row - 1,)),
                pltpu.SemaphoreType.DMA((n_row,)),
                pltpu.SemaphoreType.DMA,
                pltpu.SemaphoreType.DMA,
                pltpu.SemaphoreType.REGULAR,
                pltpu.SemaphoreType.REGULAR,
                pltpu.SemaphoreType.DMA((2,)),
            ],
            compiler_params=pltpu.CompilerParams(
                collective_id=0, has_side_effects=True, vmem_limit_bytes=60000 * 1024
            ),
        )(adjacency.T, relabel.reshape(1, n_mine))
        clustering, ratio = pl.pallas_call(
            finish,
            out_shape=(
                jax.ShapeDtypeStruct((1, n_mine), jnp.float32),
                jax.ShapeDtypeStruct((1, 1), jnp.float32),
            ),
            in_specs=[pl.BlockSpec(memory_space=pltpu.VMEM), pl.BlockSpec(memory_space=pltpu.SMEM)],
            out_specs=[pl.BlockSpec(memory_space=pl.ANY)] * 2,
            scratch_shapes=[pltpu.SemaphoreType.DMA((2,))],
        )(
            pltpu.with_memory_space_constraint(found, pltpu.VMEM),
            pltpu.with_memory_space_constraint(total, pltpu.SMEM),
        )
        return clustering.reshape(n_mine), ratio.reshape(())

    placed = (P("row", "col"), P(("row", "col")))
    return jax.shard_map(
        body, mesh=mesh, in_specs=placed, out_specs=(P(("row", "col")), P()), check_vma=False
    )
```

```python
import functools

import jax
import jax.numpy as jnp
from jax import lax
from jax.experimental import pallas as pl
from jax.experimental.pallas import tpu as pltpu
from jax.sharding import PartitionSpec as P

MESH = pl.DeviceIdType.MESH
TYPE = jnp.float8_e4m3fn


def unpack(row, times=1):
    wide = jnp.broadcast_to(row, (32, row.shape[1]))
    bits = lax.shift_right_logical(wide, lax.broadcasted_iota(jnp.int32, wide.shape, 0)) & 1
    return (bits * times).astype(jnp.int8).astype(TYPE)


def kernel(
    n_row, n_col, words_ref, relabel_ref, out_ref, total_ref,
    raw, px, py, tails, x, y, mask, hot, rel, msg, bulk, acc,
    x_send, x_recv, y_send, y_recv, m_send, m_recv, ready, go, local_sem,
):
    n_words, n_rows = words_ref.shape
    n_all = n_row * n_col
    per = n_row // n_col
    depth = 32 * n_words
    width = msg.shape[2]
    r, c = lax.axis_index("row"), lax.axis_index("col")
    barrier = pltpu.get_barrier_semaphore()
    load = pltpu.make_async_copy(words_ref, raw, local_sem.at[0])
    load_r = pltpu.make_async_copy(relabel_ref, rel, local_sem.at[1])
    load.start()
    load_r.start()
    full, half = n_rows // 128, n_rows % 128
    packed = full * n_words
    if half:
        assert half == 64 and n_words % 2 == 0 and per == 2
    if n_row & (n_row - 1) == 0:
        row_peers = [r ^ o for o in range(1, n_row)]
    else:
        row_peers = [lax.rem(r + o, n_row) for o in range(1, n_row)]
    lead = 1
    sends_y = r >= c * per
    for p in row_peers:
        @pl.when((p >= c * per) | (p == lead))
        def _():
            pl.semaphore_signal(barrier, inc=1, device_id=(p, c), device_id_type=MESH)

    def greet_above():
        for k in range(1, n_col):
            @pl.when(k > c)
            def _():
                pl.semaphore_signal(barrier, inc=1, device_id=(r, k), device_id_type=MESH)
    pl.when(r != lead)(greet_above)
    load.wait()
    for f in range(full):
        chunk = raw[:, f * 128 : (f + 1) * 128]
        px[c, f * n_words : (f + 1) * n_words, :] = chunk
        py[r, f * n_words : (f + 1) * n_words, :] = chunk
    if half:
        ends = raw[:, full * 128 :]
        ends = jnp.concatenate([ends[: n_words // 2], ends[n_words // 2 :]], axis=1)
        ends = jnp.concatenate([ends, jnp.zeros((px.shape[1] - packed - n_words // 2, 128), jnp.int32)], axis=0)
        px[c, packed:, :] = ends
        py[r, packed:, :] = ends
    pl.semaphore_wait(barrier, c + jnp.where(sends_y | (r == lead), n_row - 1, 0))

    def x_copy(p, to):
        return pltpu.make_async_remote_copy(
            px.at[p], px.at[p], x_send.at[to], x_recv.at[p], device_id=(r, to), device_id_type=MESH)

    def y_copy(p, i, to):
        return pltpu.make_async_remote_copy(
            py.at[p], py.at[p], y_send.at[i], y_recv.at[p], device_id=(to, c), device_id_type=MESH)

    for to in range(n_col - 1):
        @pl.when(to < c)
        def _():
            x_copy(c, to).start()

    @pl.when(sends_y)
    def _():
        for i, p in reversed(list(enumerate(row_peers))):
            y_copy(r, i, p).start()

    @pl.when(r == lead)
    def _():
        greet_above()
        for k in range(n_col - 1):
            @pl.when(k < c)
            def _():
                pl.semaphore_signal(ready, inc=1, device_id=(r, k), device_id_type=MESH)

    load_r.wait()
    label = rel[...]
    owner = jnp.zeros_like(label)
    for k in range(1, n_row):
        owner += (label >= k * n_rows).astype(jnp.int32)
    place = label - owner * n_rows
    hot[...] = (lax.broadcasted_iota(jnp.int32, hot.shape, 0) == place).astype(jnp.float32).astype(jnp.bfloat16)

    def at(k, w):
        b, q = divmod(w, n_rows // 32)
        if half:
            w = b * 4 * full + q if q < 4 * full else per * 4 * full + 2 * b + q - 4 * full
        return pl.ds(pl.multiple_of(k * depth + w * 32, 32), 32)

    def lanes(k, f):
        return pl.ds(pl.multiple_of(k * depth + f * 128, 128), 128)

    def take_x(k):
        times = jnp.where(k == c, 1, 2)
        if half:
            ends = px[k, packed : packed + n_words // 2, :]
            tails[0] = ends
            tails[1] = pltpu.roll(ends, 64, 1)
        for w in range(n_words):
            for f in range(full):
                x[at(k, w), f * 128 : (f + 1) * 128] = unpack(px[k, f * n_words + w : f * n_words + w + 1, :], times)
            if half:
                h, q = divmod(w, n_words // 2)
                x[at(k, w), full * 128 :] = unpack(tails[h, q : q + 1, :], times)

    def take_y(k):
        for h in range(per):
            p = k * per + h

            @pl.when(p != r)
            def _():
                y_copy(p, 0, r).wait_recv()
        if half:
            a = py[k * per, packed : packed + n_words // 2, :]
            b = py[k * per + 1, packed : packed + n_words // 2, :]
            left = lax.broadcasted_iota(jnp.int32, a.shape, 1) < 64
            tails[0] = jnp.where(left, a, pltpu.roll(b, 64, 1))
            tails[1] = jnp.where(left, pltpu.roll(a, 64, 1), b)
        for w in range(n_words):
            for h in range(per):
                for f in range(full):
                    row = py[k * per + h, f * n_words + w : f * n_words + w + 1, :]
                    y[at(0, w), lanes(k, h * full + f)] = unpack(row)
            if half:
                h, q = divmod(w, n_words // 2)
                y[at(0, w), lanes(k, per * full)] = unpack(tails[h, q : q + 1, :])

    def add(low, high):
        part = jnp.zeros((1, width), jnp.float32)
        for m in range(2):
            rows = slice(m * depth // 2, (m + 1) * depth // 2)
            paths = jnp.dot(
                y[rows, low * depth : high * depth], x[low * depth : high * depth, :],
                preferred_element_type=jnp.float32)
            part += jnp.sum(paths * mask[rows, :], axis=0, keepdims=True)
        acc[...] += part

    def wait_x(k):
        x_copy(k, 0).wait_recv()
        take_x(k)

    def hear_and_tell():
        @pl.when(c < n_col - 1)
        def _():
            pl.semaphore_wait(ready, n_col - 1 - c)
        for p in row_peers:
            pl.semaphore_signal(go, inc=1, device_id=(p, c), device_id_type=MESH)

    pl.when((r == lead) & (c == n_col - 1))(hear_and_tell)
    acc[...] = jnp.zeros_like(acc)
    take_x(c)
    mask[...] = x[pl.ds(pl.multiple_of(c * depth, 32), depth), :].astype(jnp.float32)
    own = r // per

    def step(j, carry):
        k = jnp.where(j == 0, own, n_col - j - (own >= n_col - j).astype(jnp.int32))
        pl.when(k >= c)(lambda: take_y(k))
        pl.when((j == 1) & (r == lead) & (c < n_col - 1))(hear_and_tell)
        pl.when((j > 0) & (c + j < n_col))(lambda: wait_x(c + j))
        return carry
    lax.fori_loop(0, n_col, step, 0)
    for low in range(n_col):
        @pl.when(c == low)
        def _():
            for start in range(low, n_col, 4):
                add(start, min(start + 4, n_col))

    me = c * n_row + r

    @pl.when(r != lead)
    def _():
        pl.semaphore_wait(go, 1)

    def inner(row):
        return jnp.where(lax.broadcasted_iota(jnp.int32, row.shape, 1) < n_rows, row, 0.0)

    def post(planes, to):
        mine = msg.at[planes, pl.ds(r, 1), :]
        return pltpu.make_async_remote_copy(
            mine, mine, m_send, m_recv, device_id=(lax.rem(to, n_row), to // n_row), device_id_type=MESH)

    others = [i + (i >= me).astype(jnp.int32) for i in range(n_all - 1)]

    @pl.when(c == 0)
    def _():
        count = jnp.zeros(px.shape[1:], jnp.int32)
        for k in range(n_col):
            count += lax.population_count(px[k])
        parts = [jnp.sum(count[f * n_words : (f + 1) * n_words], axis=0, keepdims=True) for f in range(full)]
        if half:
            ends = jnp.sum(count[packed : packed + n_words // 2], axis=0, keepdims=True)
            parts.append(ends + pltpu.roll(ends, 64, 1))
        degree = jnp.concatenate(parts, axis=1).astype(jnp.float32)
        wedges = jnp.maximum(degree * (degree - 1.0), 1.0)
        msg[0, pl.ds(r, 1), :] = inner(acc[...])
        msg[1, pl.ds(r, 1), :] = inner(wedges)
        for to in others:
            post(pl.ds(0, 2), to).start()

    @pl.when(c > 0)
    def _():
        msg[c + 1, pl.ds(r, 1), :] = inner(acc[...])
        for to in others:
            post(pl.ds(c + 1, 1), to).start()

    for to in range(n_col - 1):
        @pl.when(to < c)
        def _():
            x_copy(c, to).wait_send()

    @pl.when(sends_y)
    def _():
        for i, p in enumerate(row_peers):
            y_copy(r, i, p).wait_send()

    def take(rows, sem):
        pltpu.make_async_copy(bulk.at[pl.ds(0, rows)], bulk.at[pl.ds(0, rows)], sem).wait()
    pl.when(c == 0)(lambda: take(n_all - 1 + n_row - 1, m_recv))
    pl.when(c > 0)(lambda: take(n_all - 1 + n_row, m_recv))

    closed = msg[0]
    for k in range(1, n_col):
        closed += msg[k + 1]
    wedges = msg[1]
    inside = lax.broadcasted_iota(jnp.int32, closed.shape, 1) < n_rows
    ratio = jnp.where(inside, closed / wedges, 0.0)
    def whole(part):
        return jnp.sum(jnp.sum(part, axis=0, keepdims=True), axis=1, keepdims=True)
    total = whole(closed) / whole(wedges)
    total_ref[0, 0] = total[0, 0]
    high = ratio.astype(jnp.bfloat16)
    rest = ratio - high.astype(jnp.float32)
    middle = rest.astype(jnp.bfloat16)
    low = (rest - middle.astype(jnp.float32)).astype(jnp.bfloat16)
    parts = jnp.concatenate([p.astype(jnp.float32) for p in (high, middle, low)], axis=0).astype(jnp.bfloat16)
    picked = jnp.dot(parts, hot[...], preferred_element_type=jnp.float32)
    found = picked[:n_row] + picked[n_row : 2 * n_row] + picked[2 * n_row :]
    which = lax.broadcasted_iota(jnp.int32, found.shape, 0)
    out_ref[...] = jnp.sum(jnp.where(which == owner, found, 0.0), axis=0, keepdims=True)
    pl.when(c == 0)(lambda: take(2 * (n_all - 1), m_send))
    pl.when(c > 0)(lambda: take(n_all - 1, m_send))


def finish(found_ref, total_ref, out_ref, out_total_ref, sems):
    one = pltpu.make_async_copy(found_ref, out_ref, sems.at[0])
    two = pltpu.make_async_copy(total_ref, out_total_ref, sems.at[1])
    one.start()
    two.start()
    one.wait()
    two.wait()


def solution(mesh):
    n_row, n_col = mesh.shape["row"], mesh.shape["col"]
    n_all = n_row * n_col

    def body(adjacency, relabel):
        n_rows, n_words = adjacency.shape
        n_mine = relabel.shape[0]
        depth = 32 * n_words
        width = (n_rows + 127) // 128 * 128
        lines = (n_rows * n_words // 128 + 7) // 8 * 8
        found, total = pl.pallas_call(
            functools.partial(kernel, n_row, n_col),
            out_shape=(pltpu.VMEM((1, n_mine), jnp.float32), pltpu.SMEM((1, 1), jnp.float32)),
            in_specs=[pl.BlockSpec(memory_space=pl.ANY)] * 2,
            out_specs=[pl.BlockSpec(memory_space=pltpu.VMEM), pl.BlockSpec(memory_space=pltpu.SMEM)],
            scratch_shapes=[
                pltpu.VMEM((n_words, n_rows), jnp.int32),
                pltpu.VMEM((n_col, lines, 128), jnp.int32),
                pltpu.VMEM((n_row, lines, 128), jnp.int32),
                pltpu.VMEM((2, n_words // 2, 128), jnp.int32),
                pltpu.VMEM((n_col * depth, width), TYPE),
                pltpu.VMEM((depth, n_col * depth), TYPE),
                pltpu.VMEM((depth, width), jnp.float32),
                pltpu.VMEM((width, n_mine), jnp.bfloat16),
                pltpu.VMEM((1, n_mine), jnp.int32),
                pltpu.VMEM((n_col + 1, n_row, width), jnp.float32),
                pltpu.VMEM((2 * n_all, 1, width), jnp.float32),
                pltpu.VMEM((1, width), jnp.float32),
                pltpu.SemaphoreType.DMA((n_col,)),
                pltpu.SemaphoreType.DMA((n_col,)),
                pltpu.SemaphoreType.DMA((n_row - 1,)),
                pltpu.SemaphoreType.DMA((n_row,)),
                pltpu.SemaphoreType.DMA,
                pltpu.SemaphoreType.DMA,
                pltpu.SemaphoreType.REGULAR,
                pltpu.SemaphoreType.REGULAR,
                pltpu.SemaphoreType.DMA((2,)),
            ],
            compiler_params=pltpu.CompilerParams(
                collective_id=0, has_side_effects=True, vmem_limit_bytes=60000 * 1024
            ),
        )(adjacency.T, relabel.reshape(1, n_mine))
        clustering, ratio = pl.pallas_call(
            finish,
            out_shape=(
                jax.ShapeDtypeStruct((1, n_mine), jnp.float32),
                jax.ShapeDtypeStruct((1, 1), jnp.float32),
            ),
            in_specs=[pl.BlockSpec(memory_space=pltpu.VMEM), pl.BlockSpec(memory_space=pltpu.SMEM)],
            out_specs=[pl.BlockSpec(memory_space=pl.ANY)] * 2,
            scratch_shapes=[pltpu.SemaphoreType.DMA((2,))],
        )(
            pltpu.with_memory_space_constraint(found, pltpu.VMEM),
            pltpu.with_memory_space_constraint(total, pltpu.SMEM),
        )
        return clustering.reshape(n_mine), ratio.reshape(())

    placed = (P("row", "col"), P(("row", "col")))
    return jax.shard_map(
        body, mesh=mesh, in_specs=placed, out_specs=(P(("row", "col")), P()), check_vma=False
    )
```

```python
import functools

import jax
import jax.numpy as jnp
from jax import lax
from jax.experimental import pallas as pl
from jax.experimental.pallas import tpu as pltpu
from jax.sharding import PartitionSpec as P

MESH = pl.DeviceIdType.MESH
TYPE = jnp.float8_e4m3fn


def unpack(row, times=1):
    wide = jnp.broadcast_to(row, (32, row.shape[1]))
    bits = lax.shift_right_logical(wide, lax.broadcasted_iota(jnp.int32, wide.shape, 0)) & 1
    return (bits * times).astype(jnp.int8).astype(TYPE)


def kernel(
    n_row, n_col, words_ref, relabel_ref, out_ref, total_ref,
    raw, px, py, tails, x, y, mask, hot, rel, msg, bulk, acc,
    x_send, x_recv, y_send, y_recv, m_send, m_recv, ready, go, local_sem,
):
    n_words, n_rows = words_ref.shape
    n_all = n_row * n_col
    per = n_row // n_col
    depth = 32 * n_words
    width = msg.shape[2]
    r, c = lax.axis_index("row"), lax.axis_index("col")
    barrier = pltpu.get_barrier_semaphore()
    load = pltpu.make_async_copy(words_ref, raw, local_sem.at[0])
    load_r = pltpu.make_async_copy(relabel_ref, rel, local_sem.at[1])
    load.start()
    load_r.start()
    full, half = n_rows // 128, n_rows % 128
    packed = full * n_words
    tile = px.shape[2]
    if half:
        assert half == 64 and n_words % 2 == 0 and per == 2
    if n_row & (n_row - 1) == 0:
        row_peers = [r ^ o for o in range(1, n_row)]
    else:
        row_peers = [lax.rem(r + o, n_row) for o in range(1, n_row)]
    lead = 1
    sends_y = r >= c * per
    for p in row_peers:
        @pl.when((p >= c * per) | (p == lead))
        def _():
            pl.semaphore_signal(barrier, inc=1, device_id=(p, c), device_id_type=MESH)

    def greet_above():
        for k in range(1, n_col):
            @pl.when(k > c)
            def _():
                pl.semaphore_signal(barrier, inc=1, device_id=(r, k), device_id_type=MESH)
    pl.when(r != lead)(greet_above)
    load.wait()
    def keep(line, value):
        px[c, line // tile : (line + value.shape[0]) // tile] = value.reshape(-1, tile, 128)
        py[r, line // tile : (line + value.shape[0]) // tile] = value.reshape(-1, tile, 128)
    for f in range(full):
        keep(f * n_words, raw[:, f * 128 : (f + 1) * 128])
    if half:
        ends = raw[:, full * 128 :]
        keep(packed, jnp.concatenate([ends[: n_words // 2], ends[n_words // 2 :]], axis=1))
    pl.semaphore_wait(barrier, c + jnp.where(sends_y | (r == lead), n_row - 1, 0))

    def x_copy(p, to):
        return pltpu.make_async_remote_copy(
            px.at[p], px.at[p], x_send.at[to], x_recv.at[p], device_id=(r, to), device_id_type=MESH)

    def y_copy(p, i, to):
        return pltpu.make_async_remote_copy(
            py.at[p], py.at[p], y_send.at[i], y_recv.at[p], device_id=(to, c), device_id_type=MESH)

    for to in range(n_col - 1):
        @pl.when(to < c)
        def _():
            x_copy(c, to).start()

    @pl.when(sends_y)
    def _():
        for i, p in reversed(list(enumerate(row_peers))):
            y_copy(r, i, p).start()

    @pl.when(r == lead)
    def _():
        greet_above()
        for k in range(n_col - 1):
            @pl.when(k < c)
            def _():
                pl.semaphore_signal(ready, inc=1, device_id=(r, k), device_id_type=MESH)

    load_r.wait()
    label = rel[...]
    owner = jnp.zeros_like(label)
    for k in range(1, n_row):
        owner += (label >= k * n_rows).astype(jnp.int32)
    place = label - owner * n_rows
    hot[...] = (lax.broadcasted_iota(jnp.int32, hot.shape, 0) == place).astype(jnp.float32).astype(jnp.bfloat16)

    def at(k, w):
        b, q = divmod(w, n_rows // 32)
        if half:
            w = b * 4 * full + q if q < 4 * full else per * 4 * full + 2 * b + q - 4 * full
        return pl.ds(pl.multiple_of(k * depth + w * 32, 32), 32)

    def line(words, k, i):
        return words[k, i // tile, i % tile : i % tile + 1, :]

    def lines(words, k, i, n):
        return words[k, i // tile : (i + n) // tile].reshape(n, 128)

    def lanes(k, f):
        return pl.ds(pl.multiple_of(k * depth + f * 128, 128), 128)

    def take_x(k):
        times = jnp.where(k == c, 1, 2)
        if half:
            ends = lines(px, k, packed, n_words // 2)
            tails[0] = ends
            tails[1] = pltpu.roll(ends, 64, 1)
        for w in range(n_words):
            for f in range(full):
                x[at(k, w), f * 128 : (f + 1) * 128] = unpack(line(px, k, f * n_words + w), times)
            if half:
                h, q = divmod(w, n_words // 2)
                x[at(k, w), full * 128 :] = unpack(tails[h, q : q + 1, :], times)

    def take_y(k):
        for h in range(per):
            p = k * per + h

            @pl.when(p != r)
            def _():
                y_copy(p, 0, r).wait_recv()
        if half:
            a = lines(py, k * per, packed, n_words // 2)
            b = lines(py, k * per + 1, packed, n_words // 2)
            left = lax.broadcasted_iota(jnp.int32, a.shape, 1) < 64
            tails[0] = jnp.where(left, a, pltpu.roll(b, 64, 1))
            tails[1] = jnp.where(left, pltpu.roll(a, 64, 1), b)
        for w in range(n_words):
            for h in range(per):
                for f in range(full):
                    row = line(py, k * per + h, f * n_words + w)
                    y[at(0, w), lanes(k, h * full + f)] = unpack(row)
            if half:
                h, q = divmod(w, n_words // 2)
                y[at(0, w), lanes(k, per * full)] = unpack(tails[h, q : q + 1, :])

    def add(low, high):
        part = jnp.zeros((1, width), jnp.float32)
        for m in range(2):
            rows = slice(m * depth // 2, (m + 1) * depth // 2)
            paths = jnp.dot(
                y[rows, low * depth : high * depth], x[low * depth : high * depth, :],
                preferred_element_type=jnp.float32)
            part += jnp.sum(paths * mask[rows, :], axis=0, keepdims=True)
        acc[...] += part

    def wait_x(k):
        x_copy(k, 0).wait_recv()
        take_x(k)

    def hear_and_tell():
        @pl.when(c < n_col - 1)
        def _():
            pl.semaphore_wait(ready, n_col - 1 - c)
        for p in row_peers:
            pl.semaphore_signal(go, inc=1, device_id=(p, c), device_id_type=MESH)

    pl.when((r == lead) & (c == n_col - 1))(hear_and_tell)
    acc[...] = jnp.zeros_like(acc)
    take_x(c)
    mask[...] = x[pl.ds(pl.multiple_of(c * depth, 32), depth), :].astype(jnp.float32)
    own = r // per

    def step(j, carry):
        k = jnp.where(j == 0, own, n_col - j - (own >= n_col - j).astype(jnp.int32))
        pl.when(k >= c)(lambda: take_y(k))
        pl.when((j == 1) & (r == lead) & (c < n_col - 1))(hear_and_tell)
        pl.when((j > 0) & (c + j < n_col))(lambda: wait_x(c + j))
        return carry
    lax.fori_loop(0, n_col, step, 0)
    for low in range(n_col):
        @pl.when(c == low)
        def _():
            for start in range(low, n_col, 4):
                add(start, min(start + 4, n_col))

    me = c * n_row + r

    @pl.when(r != lead)
    def _():
        pl.semaphore_wait(go, 1)

    def inner(row):
        return jnp.where(lax.broadcasted_iota(jnp.int32, row.shape, 1) < n_rows, row, 0.0)

    def post(planes, to):
        mine = msg.at[planes, pl.ds(r, 1), :]
        return pltpu.make_async_remote_copy(
            mine, mine, m_send, m_recv, device_id=(lax.rem(to, n_row), to // n_row), device_id_type=MESH)

    others = [i + (i >= me).astype(jnp.int32) for i in range(n_all - 1)]

    @pl.when(c == 0)
    def _():
        count = jnp.zeros(px.shape[1:], jnp.int32)
        for k in range(n_col):
            count += lax.population_count(px[k])
        def some(low, high):
            return jnp.sum(jnp.sum(count[low // tile : high // tile], axis=0), axis=0, keepdims=True)
        parts = [some(f * n_words, (f + 1) * n_words) for f in range(full)]
        if half:
            ends = some(packed, packed + n_words // 2)
            parts.append(ends + pltpu.roll(ends, 64, 1))
        degree = jnp.concatenate(parts, axis=1).astype(jnp.float32)
        wedges = jnp.maximum(degree * (degree - 1.0), 1.0)
        msg[0, pl.ds(r, 1), :] = inner(acc[...])
        msg[1, pl.ds(r, 1), :] = inner(wedges)
        for to in others:
            post(pl.ds(0, 2), to).start()

    @pl.when(c > 0)
    def _():
        msg[c + 1, pl.ds(r, 1), :] = inner(acc[...])
        for to in others:
            post(pl.ds(c + 1, 1), to).start()

    for to in range(n_col - 1):
        @pl.when(to < c)
        def _():
            x_copy(c, to).wait_send()

    @pl.when(sends_y)
    def _():
        for i, p in enumerate(row_peers):
            y_copy(r, i, p).wait_send()

    def take(rows, sem):
        pltpu.make_async_copy(bulk.at[pl.ds(0, rows)], bulk.at[pl.ds(0, rows)], sem).wait()
    pl.when(c == 0)(lambda: take(n_all - 1 + n_row - 1, m_recv))
    pl.when(c > 0)(lambda: take(n_all - 1 + n_row, m_recv))

    closed = msg[0]
    for k in range(1, n_col):
        closed += msg[k + 1]
    wedges = msg[1]
    inside = lax.broadcasted_iota(jnp.int32, closed.shape, 1) < n_rows
    ratio = jnp.where(inside, closed / wedges, 0.0)
    def whole(part):
        return jnp.sum(jnp.sum(part, axis=0, keepdims=True), axis=1, keepdims=True)
    total = whole(closed) / whole(wedges)
    total_ref[0, 0] = total[0, 0]
    high = ratio.astype(jnp.bfloat16)
    rest = ratio - high.astype(jnp.float32)
    middle = rest.astype(jnp.bfloat16)
    low = (rest - middle.astype(jnp.float32)).astype(jnp.bfloat16)
    parts = jnp.concatenate([p.astype(jnp.float32) for p in (high, middle, low)], axis=0).astype(jnp.bfloat16)
    picked = jnp.dot(parts, hot[...], preferred_element_type=jnp.float32)
    found = picked[:n_row] + picked[n_row : 2 * n_row] + picked[2 * n_row :]
    which = lax.broadcasted_iota(jnp.int32, found.shape, 0)
    out_ref[...] = jnp.sum(jnp.where(which == owner, found, 0.0), axis=0, keepdims=True)
    pl.when(c == 0)(lambda: take(2 * (n_all - 1), m_send))
    pl.when(c > 0)(lambda: take(n_all - 1, m_send))


def finish(found_ref, total_ref, out_ref, out_total_ref, sems):
    one = pltpu.make_async_copy(found_ref, out_ref, sems.at[0])
    two = pltpu.make_async_copy(total_ref, out_total_ref, sems.at[1])
    one.start()
    two.start()
    one.wait()
    two.wait()


def solution(mesh):
    n_row, n_col = mesh.shape["row"], mesh.shape["col"]
    n_all = n_row * n_col

    def body(adjacency, relabel):
        n_rows, n_words = adjacency.shape
        n_mine = relabel.shape[0]
        depth = 32 * n_words
        width = (n_rows + 127) // 128 * 128
        lines = n_rows * n_words // 128
        tile = 2 if n_words % 4 == 0 else 1
        found, total = pl.pallas_call(
            functools.partial(kernel, n_row, n_col),
            out_shape=(pltpu.VMEM((1, n_mine), jnp.float32), pltpu.SMEM((1, 1), jnp.float32)),
            in_specs=[pl.BlockSpec(memory_space=pl.ANY)] * 2,
            out_specs=[pl.BlockSpec(memory_space=pltpu.VMEM), pl.BlockSpec(memory_space=pltpu.SMEM)],
            scratch_shapes=[
                pltpu.VMEM((n_words, n_rows), jnp.int32),
                pltpu.VMEM((n_col, lines // tile, tile, 128), jnp.int32),
                pltpu.VMEM((n_row, lines // tile, tile, 128), jnp.int32),
                pltpu.VMEM((2, n_words // 2, 128), jnp.int32),
                pltpu.VMEM((n_col * depth, width), TYPE),
                pltpu.VMEM((depth, n_col * depth), TYPE),
                pltpu.VMEM((depth, width), jnp.float32),
                pltpu.VMEM((width, n_mine), jnp.bfloat16),
                pltpu.VMEM((1, n_mine), jnp.int32),
                pltpu.VMEM((n_col + 1, n_row, width), jnp.float32),
                pltpu.VMEM((2 * n_all, 1, width), jnp.float32),
                pltpu.VMEM((1, width), jnp.float32),
                pltpu.SemaphoreType.DMA((n_col,)),
                pltpu.SemaphoreType.DMA((n_col,)),
                pltpu.SemaphoreType.DMA((n_row - 1,)),
                pltpu.SemaphoreType.DMA((n_row,)),
                pltpu.SemaphoreType.DMA,
                pltpu.SemaphoreType.DMA,
                pltpu.SemaphoreType.REGULAR,
                pltpu.SemaphoreType.REGULAR,
                pltpu.SemaphoreType.DMA((2,)),
            ],
            compiler_params=pltpu.CompilerParams(
                collective_id=0, has_side_effects=True, vmem_limit_bytes=60000 * 1024
            ),
        )(adjacency.T, relabel.reshape(1, n_mine))
        clustering, ratio = pl.pallas_call(
            finish,
            out_shape=(
                jax.ShapeDtypeStruct((1, n_mine), jnp.float32),
                jax.ShapeDtypeStruct((1, 1), jnp.float32),
            ),
            in_specs=[pl.BlockSpec(memory_space=pltpu.VMEM), pl.BlockSpec(memory_space=pltpu.SMEM)],
            out_specs=[pl.BlockSpec(memory_space=pl.ANY)] * 2,
            scratch_shapes=[pltpu.SemaphoreType.DMA((2,))],
        )(
            pltpu.with_memory_space_constraint(found, pltpu.VMEM),
            pltpu.with_memory_space_constraint(total, pltpu.SMEM),
        )
        return clustering.reshape(n_mine), ratio.reshape(())

    placed = (P("row", "col"), P(("row", "col")))
    return jax.shard_map(
        body, mesh=mesh, in_specs=placed, out_specs=(P(("row", "col")), P()), check_vma=False
    )
```

```python
import functools

import jax
import jax.numpy as jnp
from jax import lax
from jax.experimental import pallas as pl
from jax.experimental.pallas import tpu as pltpu
from jax.sharding import PartitionSpec as P

MESH = pl.DeviceIdType.MESH
TYPE = jnp.float8_e4m3fn
SPLIT = 1


def unpack(row, times=1):
    wide = jnp.broadcast_to(row, (32, row.shape[1]))
    bits = lax.shift_right_logical(wide, lax.broadcasted_iota(jnp.int32, wide.shape, 0)) & 1
    return (bits * times).astype(jnp.int8).astype(TYPE)


def kernel(
    n_row, n_col, words_ref, relabel_ref, out_ref, total_ref,
    raw, px, py, tails, x, y, mask, spot, rel, msg, bulk, acc,
    x_send, x_recv, y_send, y_recv, m_send, m_recv, ready, go, local_sem,
):
    n_words, n_rows = words_ref.shape
    n_mine = relabel_ref.shape[1]
    spare = -n_mine % 128
    n_all = n_row * n_col
    per = n_row // n_col
    depth = 32 * n_words
    width = msg.shape[2]
    r, c = lax.axis_index("row"), lax.axis_index("col")
    barrier = pltpu.get_barrier_semaphore()
    load = pltpu.make_async_copy(words_ref, raw, local_sem.at[0])
    load_r = pltpu.make_async_copy(relabel_ref, rel, local_sem.at[1])
    load.start()
    load_r.start()
    full, half = n_rows // 128, n_rows % 128
    packed = full * n_words
    tile = px.shape[2]
    if half:
        assert half == 64 and n_words % 2 == 0 and per == 2
    if n_row & (n_row - 1) == 0:
        row_peers = [r ^ 1] + [((r // 2) ^ o) * 2 + h for o in range(1, n_row // 2) for h in (1, 0)]
    else:
        row_peers = [lax.rem(r + o, n_row) for o in range(1, n_row)]
    lead = 1
    sends_y = r >= c * per
    for p in row_peers:
        @pl.when((p >= c * per) | (p == lead))
        def _():
            pl.semaphore_signal(barrier, inc=1, device_id=(p, c), device_id_type=MESH)

    def greet_above():
        for k in range(1, n_col):
            @pl.when(k > c)
            def _():
                pl.semaphore_signal(barrier, inc=1, device_id=(r, k), device_id_type=MESH)
    pl.when(r != lead)(greet_above)
    load.wait()
    def keep(line, value):
        px[c, line // tile : (line + value.shape[0]) // tile] = value.reshape(-1, tile, 128)
        py[r, line // tile : (line + value.shape[0]) // tile] = value.reshape(-1, tile, 128)
    for f in range(full):
        keep(f * n_words, raw[:, f * 128 : (f + 1) * 128])
    if half:
        ends = raw[:, full * 128 :]
        keep(packed, jnp.concatenate([ends[: n_words // 2], ends[n_words // 2 :]], axis=1))
    pl.semaphore_wait(barrier, c + jnp.where(sends_y | (r == lead), n_row - 1, 0))

    def x_copy(p, to):
        return pltpu.make_async_remote_copy(
            px.at[p], px.at[p], x_send.at[to], x_recv.at[p], device_id=(r, to), device_id_type=MESH)

    def y_copy(p, i, to):
        return pltpu.make_async_remote_copy(
            py.at[p], py.at[p], y_send.at[i], y_recv.at[p], device_id=(to, c), device_id_type=MESH)

    for to in range(n_col - 1):
        @pl.when(to < c)
        def _():
            x_copy(c, to).start()

    @pl.when(sends_y)
    def _():
        for i, p in reversed(list(enumerate(row_peers))):
            y_copy(r, i, p).start()

    @pl.when(r == lead)
    def _():
        greet_above()
        for k in range(n_col - 1):
            @pl.when(k < c)
            def _():
                pl.semaphore_signal(ready, inc=1, device_id=(r, k), device_id_type=MESH)

    load_r.wait()
    label = rel[...]
    if spare:
        label = jnp.concatenate([label, jnp.zeros((1, spare), jnp.int32)], axis=1)
    label = jnp.broadcast_to(label, (n_row, n_mine + spare))
    owner = jnp.zeros_like(label)
    for k in range(1, n_row):
        owner += (label >= k * n_rows).astype(jnp.int32)
    place = label - owner * n_rows
    mine = owner == lax.broadcasted_iota(jnp.int32, owner.shape, 0)
    spot[0] = jnp.where(mine, lax.shift_right_logical(place, 7), -1)
    spot[1] = place & 127

    above = n_col - 1 - c
    first = (above > 2).astype(jnp.int32)

    def slot(k):
        return jnp.where(k == c, 0, jnp.where((k == c + 1) & (first == 1), 1, n_col - k + first))

    def at(k, w):
        b, q = divmod(w, n_rows // 32)
        if half:
            w = b * 4 * full + q if q < 4 * full else per * 4 * full + 2 * b + q - 4 * full
        return pl.ds(pl.multiple_of(slot(k) * depth + w * 32, 32), 32)

    def line(words, k, i):
        return words[k, i // tile, i % tile : i % tile + 1, :]

    def lines(words, k, i, n):
        return words[k, i // tile : (i + n) // tile].reshape(n, 128)

    def lanes(k, f):
        return pl.ds(pl.multiple_of(slot(k) * depth + f * 128, 128), 128)

    def take_x(k):
        times = jnp.where(k == c, 1, 2)
        if half:
            ends = lines(px, k, packed, n_words // 2)
            tails[0] = ends
            tails[1] = pltpu.roll(ends, 64, 1)
        for w in range(n_words):
            for f in range(full):
                x[at(k, w), f * 128 : (f + 1) * 128] = unpack(line(px, k, f * n_words + w), times)
            if half:
                h, q = divmod(w, n_words // 2)
                x[at(k, w), full * 128 :] = unpack(tails[h, q : q + 1, :], times)

    def take_y(k):
        for h in range(per):
            p = k * per + h

            @pl.when(p != r)
            def _():
                y_copy(p, 0, r).wait_recv()
        if half:
            a = lines(py, k * per, packed, n_words // 2)
            b = lines(py, k * per + 1, packed, n_words // 2)
            left = lax.broadcasted_iota(jnp.int32, a.shape, 1) < 64
            tails[0] = jnp.where(left, a, pltpu.roll(b, 64, 1))
            tails[1] = jnp.where(left, pltpu.roll(a, 64, 1), b)
        for w in range(n_words):
            for h in range(per):
                for f in range(full):
                    row = line(py, k * per + h, f * n_words + w)
                    y[at(c, w), lanes(k, h * full + f)] = unpack(row)
            if half:
                h, q = divmod(w, n_words // 2)
                y[at(c, w), lanes(k, per * full)] = unpack(tails[h, q : q + 1, :])

    def add(low, high):
        part = jnp.zeros((1, width), jnp.float32)
        for m in range(SPLIT):
            rows = slice(m * depth // SPLIT, (m + 1) * depth // SPLIT)
            paths = jnp.dot(
                y[rows, low * depth : high * depth], x[low * depth : high * depth, :],
                preferred_element_type=jnp.float32)
            part += jnp.sum(paths * mask[rows, :], axis=0, keepdims=True)
        acc[...] += part

    def wait_x(k):
        x_copy(k, 0).wait_recv()
        take_x(k)

    def hear_and_tell():
        @pl.when(c < n_col - 1)
        def _():
            pl.semaphore_wait(ready, n_col - 1 - c)
        for p in row_peers:
            pl.semaphore_signal(go, inc=1, device_id=(p, c), device_id_type=MESH)

    pl.when((r == lead) & (c == n_col - 1))(hear_and_tell)
    acc[...] = jnp.zeros_like(acc)
    take_x(c)
    mask[...] = x[0:depth, :].astype(jnp.float32)
    own = r // per

    def next_y(j, carry):
        k = jnp.where(j == 0, own, n_col - j - (own >= n_col - j).astype(jnp.int32))
        pl.when(k >= c)(lambda: take_y(k))
        pl.when((j == 1) & (r == lead) & (c < n_col - 1))(hear_and_tell)
        return carry
    lax.fori_loop(0, n_col, next_y, 0)

    def next_x(j, carry):
        wait_x(jnp.where((j == 1) & (first == 1), c + 1, n_col - j + first))
        return carry

    def inner(row):
        return jnp.where(lax.broadcasted_iota(jnp.int32, row.shape, 1) < n_rows, row, 0.0)

    for rest in range(n_col):
        @pl.when(above == rest)
        def _():
            early = rest if rest > 1 else rest + 1
            lax.fori_loop(1, early, next_x, 0)
            for start in range(0, early, 4):
                add(start, min(start + 4, early))
            if early <= rest:
                next_x(rest, 0)
                add(rest, rest + 1)

    @pl.when(c == 0)
    def _():
        count = jnp.zeros(px.shape[1:], jnp.int32)
        for k in range(n_col):
            count += lax.population_count(px[k])
        def some(low, high):
            return jnp.sum(jnp.sum(count[low // tile : high // tile], axis=0), axis=0, keepdims=True)
        parts = [some(f * n_words, (f + 1) * n_words) for f in range(full)]
        if half:
            ends = some(packed, packed + n_words // 2)
            parts.append(ends + pltpu.roll(ends, 64, 1))
        degree = jnp.concatenate(parts, axis=1).astype(jnp.float32)
        wedges = jnp.maximum(degree * (degree - 1.0), 1.0)
        msg[1, pl.ds(r, 1), :] = inner(wedges)

    me = c * n_row + r

    @pl.when(r != lead)
    def _():
        pl.semaphore_wait(go, 1)

    def post(planes, to):
        mine = msg.at[planes, pl.ds(r, 1), :]
        return pltpu.make_async_remote_copy(
            mine, mine, m_send, m_recv, device_id=(lax.rem(to, n_row), to // n_row), device_id_type=MESH)

    others = [i + (i >= me).astype(jnp.int32) for i in range(n_all - 1)]

    @pl.when(c == 0)
    def _():
        msg[0, pl.ds(r, 1), :] = inner(acc[...])
        for to in others:
            post(pl.ds(0, 2), to).start()

    @pl.when(c > 0)
    def _():
        msg[c + 1, pl.ds(r, 1), :] = inner(acc[...])
        for to in others:
            post(pl.ds(c + 1, 1), to).start()

    for to in range(n_col - 1):
        @pl.when(to < c)
        def _():
            x_copy(c, to).wait_send()

    @pl.when(sends_y)
    def _():
        for i, p in enumerate(row_peers):
            y_copy(r, i, p).wait_send()

    def take(rows, sem):
        pltpu.make_async_copy(bulk.at[pl.ds(0, rows)], bulk.at[pl.ds(0, rows)], sem).wait()
    pl.when(c == 0)(lambda: take(n_all - 1 + n_row - 1, m_recv))
    pl.when(c > 0)(lambda: take(n_all - 1 + n_row, m_recv))

    closed = msg[0]
    for k in range(1, n_col):
        closed += msg[k + 1]
    wedges = msg[1]
    inside = lax.broadcasted_iota(jnp.int32, closed.shape, 1) < n_rows
    ratio = jnp.where(inside, closed / wedges, 0.0)
    def whole(part):
        return jnp.sum(jnp.sum(part, axis=0, keepdims=True), axis=1, keepdims=True)
    total = whole(closed) / whole(wedges)
    total_ref[0, 0] = total[0, 0]
    for m in range(0, n_mine, 128):
        chunk, lane = spot[0, :, m : m + 128], spot[1, :, m : m + 128]
        found = jnp.zeros((n_row, 128), jnp.float32)
        for f in range(width // 128):
            picked = jnp.take_along_axis(ratio[:, f * 128 : (f + 1) * 128], lane, axis=1)
            found += jnp.where(chunk == f, picked, 0.0)
        end = min(m + 128, n_mine)
        out_ref[:, m:end] = jnp.sum(found, axis=0, keepdims=True)[:, : end - m]
    pl.when(c == 0)(lambda: take(2 * (n_all - 1), m_send))
    pl.when(c > 0)(lambda: take(n_all - 1, m_send))


def finish(found_ref, total_ref, out_ref, out_total_ref, sems):
    one = pltpu.make_async_copy(found_ref, out_ref, sems.at[0])
    two = pltpu.make_async_copy(total_ref, out_total_ref, sems.at[1])
    one.start()
    two.start()
    one.wait()
    two.wait()


def solution(mesh):
    n_row, n_col = mesh.shape["row"], mesh.shape["col"]
    n_all = n_row * n_col

    def body(adjacency, relabel):
        n_rows, n_words = adjacency.shape
        n_mine = relabel.shape[0]
        depth = 32 * n_words
        width = (n_rows + 127) // 128 * 128
        lines = n_rows * n_words // 128
        tile = 2 if n_words % 4 == 0 else 1
        found, total = pl.pallas_call(
            functools.partial(kernel, n_row, n_col),
            out_shape=(pltpu.VMEM((1, n_mine), jnp.float32), pltpu.SMEM((1, 1), jnp.float32)),
            in_specs=[pl.BlockSpec(memory_space=pl.ANY)] * 2,
            out_specs=[pl.BlockSpec(memory_space=pltpu.VMEM), pl.BlockSpec(memory_space=pltpu.SMEM)],
            scratch_shapes=[
                pltpu.VMEM((n_words, n_rows), jnp.int32),
                pltpu.VMEM((n_col, lines // tile, tile, 128), jnp.int32),
                pltpu.VMEM((n_row, lines // tile, tile, 128), jnp.int32),
                pltpu.VMEM((2, n_words // 2, 128), jnp.int32),
                pltpu.VMEM((n_col * depth, width), TYPE),
                pltpu.VMEM((depth, n_col * depth), TYPE),
                pltpu.VMEM((depth, width), jnp.float32),
                pltpu.VMEM((2, n_row, n_mine + -n_mine % 128), jnp.int32),
                pltpu.VMEM((1, n_mine), jnp.int32),
                pltpu.VMEM((n_col + 1, n_row, width), jnp.float32),
                pltpu.VMEM((2 * n_all, 1, width), jnp.float32),
                pltpu.VMEM((1, width), jnp.float32),
                pltpu.SemaphoreType.DMA((n_col,)),
                pltpu.SemaphoreType.DMA((n_col,)),
                pltpu.SemaphoreType.DMA((n_row - 1,)),
                pltpu.SemaphoreType.DMA((n_row,)),
                pltpu.SemaphoreType.DMA,
                pltpu.SemaphoreType.DMA,
                pltpu.SemaphoreType.REGULAR,
                pltpu.SemaphoreType.REGULAR,
                pltpu.SemaphoreType.DMA((2,)),
            ],
            compiler_params=pltpu.CompilerParams(
                collective_id=0, has_side_effects=True, vmem_limit_bytes=60000 * 1024
            ),
        )(adjacency.T, relabel.reshape(1, n_mine))
        clustering, ratio = pl.pallas_call(
            finish,
            out_shape=(
                jax.ShapeDtypeStruct((1, n_mine), jnp.float32),
                jax.ShapeDtypeStruct((1, 1), jnp.float32),
            ),
            in_specs=[pl.BlockSpec(memory_space=pltpu.VMEM), pl.BlockSpec(memory_space=pltpu.SMEM)],
            out_specs=[pl.BlockSpec(memory_space=pl.ANY)] * 2,
            scratch_shapes=[pltpu.SemaphoreType.DMA((2,))],
        )(
            pltpu.with_memory_space_constraint(found, pltpu.VMEM),
            pltpu.with_memory_space_constraint(total, pltpu.SMEM),
        )
        return clustering.reshape(n_mine), ratio.reshape(())

    placed = (P("row", "col"), P(("row", "col")))
    return jax.shard_map(
        body, mesh=mesh, in_specs=placed, out_specs=(P(("row", "col")), P()), check_vma=False
    )
```

```python
import functools

import jax
import jax.numpy as jnp
from jax import lax
from jax.experimental import pallas as pl
from jax.experimental.pallas import tpu as pltpu
from jax.sharding import PartitionSpec as P

MESH = pl.DeviceIdType.MESH
TYPE = jnp.float8_e4m3fn


def unpack(row, times=1):
    wide = jnp.broadcast_to(row, (32, row.shape[1]))
    bits = lax.shift_right_logical(wide, lax.broadcasted_iota(jnp.int32, wide.shape, 0)) & 1
    return (bits * times).astype(jnp.int8).astype(TYPE)


def kernel(
    n_row, n_col, words_ref, relabel_ref, out_ref, total_ref,
    raw, both, px, py, x, y, own, mask, spot, rel, msg, bulk,
    b_send, b_recv, x_send, x_recv, y_send, y_recv, m_send, m_recv, ready, go, local_sem,
):
    n_words, n_rows = words_ref.shape
    n_mine = relabel_ref.shape[1]
    spare = -n_mine % 128
    n_all = n_row * n_col
    assert n_row == 2 * n_col and n_words % 4 == 0 and n_rows % 64 == 0
    depth = 32 * n_words
    nw = n_words // 2
    full, half = n_rows // 128, n_rows % 128
    packed = full * nw
    stride = y.shape[1] // n_col
    width, n_sub = msg.shape[3], msg.shape[2]
    r, c = lax.axis_index("row"), lax.axis_index("col")
    q, h = r // 2, lax.rem(r, 2)
    pair = r + 1 - 2 * h
    barrier = pltpu.get_barrier_semaphore()
    load = pltpu.make_async_copy(words_ref, raw, local_sem.at[0])
    load_r = pltpu.make_async_copy(relabel_ref, rel, local_sem.at[1])
    load.start()
    load_r.start()
    lead = 1
    sends_y = q >= c
    for o in range(1, n_row):
        p = lax.rem(r + o, n_row)

        @pl.when((p == pair) | ((lax.rem(p, 2) == h) & (p // 2 >= c)) | (p == lead))
        def _():
            pl.semaphore_signal(barrier, inc=1, device_id=(p, c), device_id_type=MESH)

    def greet_above():
        for k in range(1, n_col):
            @pl.when(k > c)
            def _():
                for e in range(2):
                    pl.semaphore_signal(barrier, inc=1, device_id=(2 * q + e, k), device_id_type=MESH)
    pl.when(r != lead)(greet_above)
    load.wait()
    for e in range(2):
        for w in range(nw):
            for f in range(full):
                both[h, e, f * nw + w] = raw[e * nw + w : e * nw + w + 1, f * 128 : (f + 1) * 128]
        if half:
            for t in range(nw // 2):
                two = [raw[e * nw + t + d : e * nw + t + d + 1, full * 128 :] for d in (0, nw // 2)]
                both[h, e, packed + t] = jnp.concatenate(two, axis=1)
    in_plane = jnp.where(r == lead, n_row - 1, jnp.where(sends_y, n_col, 1))
    pl.semaphore_wait(barrier, 2 * c + in_plane)

    def x_copy(k, e, to):
        return pltpu.make_async_remote_copy(
            both.at[h, e], px.at[k, h], x_send.at[to, e], x_recv.at[k, h],
            device_id=(2 * q + e, to), device_id_type=MESH)

    def y_copy(k, o):
        to = 2 * lax.rem(q + o, n_col) + h
        return pltpu.make_async_remote_copy(
            both.at[h], py.at[k], y_send.at[o], y_recv.at[k], device_id=(to, c), device_id_type=MESH)

    swap = pltpu.make_async_remote_copy(
        both.at[h], both.at[h], b_send, b_recv, device_id=(pair, c), device_id_type=MESH)

    for to in range(n_col - 1):
        @pl.when(to < c)
        def _():
            for e in range(2):
                x_copy(c, e, to).start()

    @pl.when(sends_y)
    def _():
        for o in range(n_col - 1, 0, -1):
            y_copy(q, o).start()
    swap.start()

    @pl.when(r == lead)
    def _():
        greet_above()
        for k in range(n_col - 1):
            @pl.when(k < c)
            def _():
                pl.semaphore_signal(ready, inc=1, device_id=(r, k), device_id_type=MESH)

    py[q] = both[h]
    if n_sub > n_col:
        for p in range(n_col + 1):
            for e in range(2):
                msg[p, e, n_col:, :] = jnp.zeros((n_sub - n_col, width), jnp.float32)
    if half:
        for k in range(n_col):
            x[k * stride + n_rows : (k + 1) * stride, :] = jnp.zeros((stride - n_rows, width), TYPE)
    load_r.wait()
    label = rel[...]
    if spare:
        label = jnp.concatenate([label, jnp.zeros((1, spare), jnp.int32)], axis=1)
    label = jnp.broadcast_to(label, (n_sub, n_mine + spare))
    owner = jnp.zeros_like(label)
    for k in range(1, n_row):
        owner += (label >= k * n_rows).astype(jnp.int32)
    place = label - owner * n_rows
    part = owner & 1
    lane = jnp.where(
        place < full * 128, part * (full * 128) + place, full * 128 + part * 64 + place)
    mine = lax.shift_right_logical(owner, 1) == lax.broadcasted_iota(jnp.int32, owner.shape, 0)
    spot[0] = jnp.where(mine, lax.shift_right_logical(lane, 7), -1)
    spot[1] = lane & 127

    above = n_col - 1 - c
    first = (above > 2).astype(jnp.int32)

    def slot(k):
        return jnp.where(k == c, 0, jnp.where((k == c + 1) & (first == 1), 1, n_col - k + first))

    left = lax.broadcasted_iota(jnp.int32, (1, 128), 1) < 64

    def spread(a, b, into, start, times):
        ends = [None] * nw
        if half:
            for t in range(nw // 2):
                one, two = a(packed + t), b(packed + t)
                ends[t] = jnp.where(left, one, pltpu.roll(two, 64, 1))
                ends[t + nw // 2] = jnp.where(left, pltpu.roll(one, 64, 1), two)
        for w in range(nw):
            rows = pl.ds(pl.multiple_of(start + w * 32, 32), 32)
            for e, get in enumerate((a, b)):
                for f in range(full):
                    at = (e * full + f) * 128
                    into[rows, at : at + 128] = unpack(get(f * nw + w), times)
            if half:
                into[rows, 2 * full * 128 :] = unpack(ends[w], times)

    def take_x(k):
        for e in range(2):
            pltpu.make_async_remote_copy(
                px.at[k, e], px.at[k, e], x_send.at[0, 0], x_recv.at[k, e],
                device_id=(r, 0), device_id_type=MESH).wait_recv()
        spread(lambda i: px[k, 0, i], lambda i: px[k, 1, i], x, slot(k) * stride, 2)

    def take_y(k):
        @pl.when(k != q)
        def _():
            pltpu.make_async_remote_copy(
                py.at[k], py.at[k], y_send.at[0], y_recv.at[k], device_id=(r, c), device_id_type=MESH).wait_recv()

        def lanes(f):
            return pl.ds(pl.multiple_of(slot(k) * stride + f * 128, 128), 128)
        for e in range(2):
            for w in range(nw):
                rows = slice((e * nw + w) * 32, (e * nw + w + 1) * 32)
                for f in range(full):
                    y[rows, lanes(f)] = unpack(py[k, e, f * nw + w])
                if half:
                    ends = py[k, e, packed + w % (nw // 2)]
                    y[rows, lanes(full)] = unpack(ends if w < nw // 2 else pltpu.roll(ends, 64, 1))

    def hear_and_tell():
        @pl.when(c < n_col - 1)
        def _():
            pl.semaphore_wait(ready, n_col - 1 - c)
        for o in range(1, n_row):
            pl.semaphore_signal(go, inc=1, device_id=(lax.rem(r + o, n_row), c), device_id_type=MESH)

    pl.when((r == lead) & (c == n_col - 1))(hear_and_tell)
    swap.wait_recv()
    for e in range(2):
        spread(lambda i: both[0, e, i], lambda i: both[1, e, i], own, e * n_rows, 1)
    mask[...] = own[...].astype(jnp.float32)
    x[0:n_rows, :] = own[pl.ds(pl.multiple_of(h * n_rows, 32), n_rows), :]

    def next_y(j, carry):
        k = jnp.where(j == 0, q, n_col - j - (q >= n_col - j).astype(jnp.int32))
        pl.when(k >= c)(lambda: take_y(k))
        pl.when((j == 1) & (r == lead) & (c < n_col - 1))(hear_and_tell)
        return carry
    lax.fori_loop(0, n_col, next_y, 0)

    def next_x(j, carry):
        take_x(jnp.where((j == 1) & (first == 1), c + 1, n_col - j + first))
        return carry
    lax.fori_loop(1, above + 1, next_x, 0)

    def degrees():
        sums = []
        for e in range(2):
            count = lax.population_count(both[e, h])
            for k in range(1, n_col):
                count += lax.population_count(px[k, e])
            sums.append([jnp.sum(count[f * nw : (f + 1) * nw], axis=0) for f in range(full)])
            if half:
                ends = jnp.sum(count[packed:], axis=0)
                sums[e].append(ends + pltpu.roll(ends, 64, 1))
        lines = sums[0][:full] + sums[1][:full]
        if half:
            lines.append(jnp.where(left, sums[0][full], sums[1][full]))
        return jnp.concatenate(lines, axis=1).astype(jnp.float32)

    for last in range(n_col):
        @pl.when(above == last)
        def _():
            low = n_col - 1 - last
            if low == 0:
                msg[1, h, pl.ds(q, 1), :] = degrees()
            part = jnp.zeros((1, width), jnp.float32)
            for s in range(0, last + 1, 4):
                span = slice(s * stride, min(s + 4, last + 1) * stride)
                paths = jnp.dot(y[:, span], x[span, :], preferred_element_type=jnp.float32)
                part += jnp.sum(paths * mask[...], axis=0, keepdims=True)
            msg[low + 1 if low else 0, h, pl.ds(q, 1), :] = part

    me = c * n_row + r

    @pl.when(r != lead)
    def _():
        pl.semaphore_wait(go, 1)

    def post(planes, to):
        mine = msg.at[planes, h, pl.ds(q, 1), :]
        return pltpu.make_async_remote_copy(
            mine, mine, m_send, m_recv, device_id=(lax.rem(to, n_row), to // n_row), device_id_type=MESH)

    others = [i + (i >= me).astype(jnp.int32) for i in range(n_all - 1)]

    @pl.when(c == 0)
    def _():
        for to in others:
            post(pl.ds(0, 2), to).start()

    @pl.when(c > 0)
    def _():
        for to in others:
            post(pl.ds(c + 1, 1), to).start()

    for to in range(n_col - 1):
        @pl.when(to < c)
        def _():
            for e in range(2):
                x_copy(c, e, to).wait_send()

    @pl.when(sends_y)
    def _():
        for o in range(1, n_col):
            y_copy(q, o).wait_send()
    swap.wait_send()

    def take(rows, sem):
        pltpu.make_async_copy(bulk.at[pl.ds(0, rows)], bulk.at[pl.ds(0, rows)], sem).wait()
    pl.when(c == 0)(lambda: take(n_all - 1 + n_row - 1, m_recv))
    pl.when(c > 0)(lambda: take(n_all - 1 + n_row, m_recv))

    closed = sum(msg[p, e] for p in range(n_col + 1) if p != 1 for e in range(2))
    degree = msg[1, 0] + msg[1, 1]
    wedges = jnp.maximum(degree * (degree - 1.0), 1.0)
    ratio = closed / wedges
    wedges = jnp.where(lax.broadcasted_iota(jnp.int32, wedges.shape, 0) < n_col, wedges, 0.0)

    def whole(part):
        return jnp.sum(jnp.sum(part, axis=0, keepdims=True), axis=1, keepdims=True)
    total = whole(closed) / whole(wedges)
    total_ref[0, 0] = total[0, 0]
    for m in range(0, n_mine, 128):
        chunk, lane = spot[0, :, m : m + 128], spot[1, :, m : m + 128]
        found = jnp.zeros((n_sub, 128), jnp.float32)
        for f in range(width // 128):
            picked = jnp.take_along_axis(ratio[:, f * 128 : (f + 1) * 128], lane, axis=1)
            found += jnp.where(chunk == f, picked, 0.0)
        end = min(m + 128, n_mine)
        out_ref[:, m:end] = jnp.sum(found, axis=0, keepdims=True)[:, : end - m]
    pl.when(c == 0)(lambda: take(2 * (n_all - 1), m_send))
    pl.when(c > 0)(lambda: take(n_all - 1, m_send))


def finish(found_ref, total_ref, out_ref, out_total_ref, sems):
    one = pltpu.make_async_copy(found_ref, out_ref, sems.at[0])
    two = pltpu.make_async_copy(total_ref, out_total_ref, sems.at[1])
    one.start()
    two.start()
    one.wait()
    two.wait()


def solution(mesh):
    n_row, n_col = mesh.shape["row"], mesh.shape["col"]
    n_all = n_row * n_col

    def body(adjacency, relabel):
        n_rows, n_words = adjacency.shape
        n_mine = relabel.shape[0]
        depth = 32 * n_words
        width = 2 * n_rows
        lines = n_rows * n_words // 256
        stride = (n_rows + 127) // 128 * 128
        n_sub = max(8, n_col)
        found, total = pl.pallas_call(
            functools.partial(kernel, n_row, n_col),
            out_shape=(pltpu.VMEM((1, n_mine), jnp.float32), pltpu.SMEM((1, 1), jnp.float32)),
            in_specs=[pl.BlockSpec(memory_space=pl.ANY)] * 2,
            out_specs=[pl.BlockSpec(memory_space=pltpu.VMEM), pl.BlockSpec(memory_space=pltpu.SMEM)],
            scratch_shapes=[
                pltpu.VMEM((n_words, n_rows), jnp.int32),
                pltpu.VMEM((2, 2, lines, 1, 128), jnp.int32),
                pltpu.VMEM((n_col, 2, lines, 1, 128), jnp.int32),
                pltpu.VMEM((n_col, 2, lines, 1, 128), jnp.int32),
                pltpu.VMEM((n_col * stride, width), TYPE),
                pltpu.VMEM((depth, n_col * stride), TYPE),
                pltpu.VMEM((depth, width), TYPE),
                pltpu.VMEM((depth, width), jnp.float32),
                pltpu.VMEM((2, n_sub, n_mine + -n_mine % 128), jnp.int32),
                pltpu.VMEM((1, n_mine), jnp.int32),
                pltpu.VMEM((n_col + 1, 2, n_sub, width), jnp.float32),
                pltpu.VMEM((2 * n_all, 1, width), jnp.float32),
                pltpu.SemaphoreType.DMA,
                pltpu.SemaphoreType.DMA,
                pltpu.SemaphoreType.DMA((n_col, 2)),
                pltpu.SemaphoreType.DMA((n_col, 2)),
                pltpu.SemaphoreType.DMA((n_col,)),
                pltpu.SemaphoreType.DMA((n_col,)),
                pltpu.SemaphoreType.DMA,
                pltpu.SemaphoreType.DMA,
                pltpu.SemaphoreType.REGULAR,
                pltpu.SemaphoreType.REGULAR,
                pltpu.SemaphoreType.DMA((2,)),
            ],
            compiler_params=pltpu.CompilerParams(
                collective_id=0, has_side_effects=True, vmem_limit_bytes=60000 * 1024
            ),
        )(adjacency.T, relabel.reshape(1, n_mine))
        clustering, ratio = pl.pallas_call(
            finish,
            out_shape=(
                jax.ShapeDtypeStruct((1, n_mine), jnp.float32),
                jax.ShapeDtypeStruct((1, 1), jnp.float32),
            ),
            in_specs=[pl.BlockSpec(memory_space=pltpu.VMEM), pl.BlockSpec(memory_space=pltpu.SMEM)],
            out_specs=[pl.BlockSpec(memory_space=pl.ANY)] * 2,
            scratch_shapes=[pltpu.SemaphoreType.DMA((2,))],
        )(
            pltpu.with_memory_space_constraint(found, pltpu.VMEM),
            pltpu.with_memory_space_constraint(total, pltpu.SMEM),
        )
        return clustering.reshape(n_mine), ratio.reshape(())

    placed = (P("row", "col"), P(("row", "col")))
    return jax.shard_map(
        body, mesh=mesh, in_specs=placed, out_specs=(P(("row", "col")), P()), check_vma=False
    )
```

```python
import functools

import jax
import jax.numpy as jnp
from jax import lax
from jax.experimental import pallas as pl
from jax.experimental.pallas import tpu as pltpu
from jax.sharding import PartitionSpec as P

MESH = pl.DeviceIdType.MESH
TYPE = jnp.float8_e4m3fn


def unpack(row, times=1):
    wide = jnp.broadcast_to(row, (32, row.shape[1]))
    bits = lax.shift_right_logical(wide, lax.broadcasted_iota(jnp.int32, wide.shape, 0)) & 1
    return (bits * times).astype(jnp.int8).astype(TYPE)


def kernel(
    n_row, n_col, words_ref, relabel_ref, out_ref, total_ref,
    raw, both, px, py, x, y, own, mask, spot, rel, msg, bulk,
    b_send, b_recv, x_send, x_recv, y_send, y_recv, m_send, m_recv, here, ready, go, local_sem,
):
    n_words, n_rows = words_ref.shape
    n_mine = relabel_ref.shape[1]
    spare = -n_mine % 128
    n_all = n_row * n_col
    assert n_row == 2 * n_col and n_words % 4 == 0 and n_rows % 64 == 0
    depth = 32 * n_words
    nw = n_words // 2
    full, half = n_rows // 128, n_rows % 128
    packed = full * nw
    stride = y.shape[1] // n_col
    width, n_sub = msg.shape[3], msg.shape[2]
    r, c = lax.axis_index("row"), lax.axis_index("col")
    q, h = r // 2, lax.rem(r, 2)
    pair = r + 1 - 2 * h
    barrier = pltpu.get_barrier_semaphore()
    load = pltpu.make_async_copy(words_ref, raw, local_sem.at[0])
    load_r = pltpu.make_async_copy(relabel_ref, rel, local_sem.at[1])
    load.start()
    load_r.start()
    lead = 1
    sends_y = q >= c
    for o in range(1, n_row):
        p = lax.rem(r + o, n_row)

        @pl.when((p == pair) | ((lax.rem(p, 2) == h) & (p // 2 >= c)) | (r == lead))
        def _():
            pl.semaphore_signal(barrier, inc=1, device_id=(p, c), device_id_type=MESH)

    def greet_above():
        for k in range(1, n_col):
            @pl.when(k > c)
            def _():
                for e in range(2):
                    pl.semaphore_signal(barrier, inc=1, device_id=(2 * q + e, k), device_id_type=MESH)
    greet_above()
    load.wait()
    for e in range(2):
        for w in range(nw):
            for f in range(full):
                both[h, e, f * nw + w] = raw[e * nw + w : e * nw + w + 1, f * 128 : (f + 1) * 128]
        if half:
            for t in range(nw // 2):
                two = [raw[e * nw + t + d : e * nw + t + d + 1, full * 128 :] for d in (0, nw // 2)]
                both[h, e, packed + t] = jnp.concatenate(two, axis=1)
    known = (r == lead) | (pair == lead) | (sends_y & (h == lead % 2))
    pl.semaphore_wait(barrier, 2 * c + jnp.where(sends_y, n_col, 1) + jnp.where(known, 0, 1))

    def x_copy(k, e, to):
        return pltpu.make_async_remote_copy(
            both.at[h, e], px.at[k, h], x_send.at[to, e], x_recv.at[k, h],
            device_id=(2 * q + e, to), device_id_type=MESH)

    def y_copy(k, o):
        to = 2 * lax.rem(q + o, n_col) + h
        return pltpu.make_async_remote_copy(
            both.at[h], py.at[k], y_send.at[o], y_recv.at[k], device_id=(to, c), device_id_type=MESH)

    swap = pltpu.make_async_remote_copy(
        both.at[h], both.at[h], b_send, b_recv, device_id=(pair, c), device_id_type=MESH)

    for to in range(n_col - 1):
        @pl.when(to < c)
        def _():
            for e in range(2):
                x_copy(c, e, to).start()

    @pl.when(sends_y)
    def _():
        for o in range(n_col - 1, 0, -1):
            y_copy(q, o).start()
    swap.start()

    @pl.when(r != lead)
    def _():
        pl.semaphore_signal(here, inc=1, device_id=(lead, c), device_id_type=MESH)

    py[q] = both[h]
    if n_sub > n_col:
        for p in range(n_col + 1):
            for e in range(2):
                msg[p, e, n_col:, :] = jnp.zeros((n_sub - n_col, width), jnp.float32)
    if half:
        for k in range(n_col):
            x[k * stride + n_rows : (k + 1) * stride, :] = jnp.zeros((stride - n_rows, width), TYPE)
    load_r.wait()
    label = rel[...]
    if spare:
        label = jnp.concatenate([label, jnp.zeros((1, spare), jnp.int32)], axis=1)
    label = jnp.broadcast_to(label, (n_sub, n_mine + spare))
    owner = jnp.zeros_like(label)
    for k in range(1, n_row):
        owner += (label >= k * n_rows).astype(jnp.int32)
    place = label - owner * n_rows
    part = owner & 1
    lane = jnp.where(
        place < full * 128, part * (full * 128) + place, full * 128 + part * 64 + place)
    mine = lax.shift_right_logical(owner, 1) == lax.broadcasted_iota(jnp.int32, owner.shape, 0)
    spot[0] = jnp.where(mine, lax.shift_right_logical(lane, 7), -1)
    spot[1] = lane & 127

    above = n_col - 1 - c
    first = (above > 2).astype(jnp.int32)

    def slot(k):
        return jnp.where(k == c, 0, jnp.where((k == c + 1) & (first == 1), 1, n_col - k + first))

    left = lax.broadcasted_iota(jnp.int32, (1, 128), 1) < 64

    def spread(a, b, into, start, times):
        ends = [None] * nw
        if half:
            for t in range(nw // 2):
                one, two = a(packed + t), b(packed + t)
                ends[t] = jnp.where(left, one, pltpu.roll(two, 64, 1))
                ends[t + nw // 2] = jnp.where(left, pltpu.roll(one, 64, 1), two)
        for w in range(nw):
            rows = pl.ds(pl.multiple_of(start + w * 32, 32), 32)
            for e, get in enumerate((a, b)):
                for f in range(full):
                    at = (e * full + f) * 128
                    into[rows, at : at + 128] = unpack(get(f * nw + w), times)
            if half:
                into[rows, 2 * full * 128 :] = unpack(ends[w], times)

    def take_x(k):
        for e in range(2):
            pltpu.make_async_remote_copy(
                px.at[k, e], px.at[k, e], x_send.at[0, 0], x_recv.at[k, e],
                device_id=(r, 0), device_id_type=MESH).wait_recv()
        spread(lambda i: px[k, 0, i], lambda i: px[k, 1, i], x, slot(k) * stride, 2)

    def take_y(k):
        @pl.when(k != q)
        def _():
            pltpu.make_async_remote_copy(
                py.at[k], py.at[k], y_send.at[0], y_recv.at[k], device_id=(r, c), device_id_type=MESH).wait_recv()

        def lanes(f):
            return pl.ds(pl.multiple_of(slot(k) * stride + f * 128, 128), 128)
        for e in range(2):
            for w in range(nw):
                rows = slice((e * nw + w) * 32, (e * nw + w + 1) * 32)
                for f in range(full):
                    y[rows, lanes(f)] = unpack(py[k, e, f * nw + w])
                if half:
                    ends = py[k, e, packed + w % (nw // 2)]
                    y[rows, lanes(full)] = unpack(ends if w < nw // 2 else pltpu.roll(ends, 64, 1))

    def hear():
        pl.semaphore_wait(here, n_row - 1)
        for k in range(n_col - 1):
            @pl.when(k < c)
            def _():
                pl.semaphore_signal(ready, inc=1, device_id=(r, k), device_id_type=MESH)
        pl.when(c == n_col - 1)(tell)

    def tell():
        @pl.when(c < n_col - 1)
        def _():
            pl.semaphore_wait(ready, n_col - 1 - c)
        for o in range(1, n_row):
            pl.semaphore_signal(go, inc=1, device_id=(lax.rem(r + o, n_row), c), device_id_type=MESH)

    swap.wait_recv()
    for e in range(2):
        spread(lambda i: both[0, e, i], lambda i: both[1, e, i], own, e * n_rows, 1)
    mask[...] = own[...].astype(jnp.float32)
    x[0:n_rows, :] = own[pl.ds(pl.multiple_of(h * n_rows, 32), n_rows), :]

    def next_y(j, carry):
        k = jnp.where(j == 0, q, n_col - j - (q >= n_col - j).astype(jnp.int32))
        pl.when(k >= c)(lambda: take_y(k))
        return carry
    pl.when(r == lead)(hear)
    lax.fori_loop(0, n_col, next_y, 0)

    def next_x(j, carry):
        pl.when((j == above) & (r == lead))(tell)
        take_x(jnp.where((j == 1) & (first == 1), c + 1, n_col - j + first))
        return carry
    lax.fori_loop(1, above + 1, next_x, 0)

    def degrees():
        sums = []
        for e in range(2):
            count = lax.population_count(both[e, h])
            for k in range(1, n_col):
                count += lax.population_count(px[k, e])
            sums.append([jnp.sum(count[f * nw : (f + 1) * nw], axis=0) for f in range(full)])
            if half:
                ends = jnp.sum(count[packed:], axis=0)
                sums[e].append(ends + pltpu.roll(ends, 64, 1))
        lines = sums[0][:full] + sums[1][:full]
        if half:
            lines.append(jnp.where(left, sums[0][full], sums[1][full]))
        return jnp.concatenate(lines, axis=1).astype(jnp.float32)

    for last in range(n_col):
        @pl.when(above == last)
        def _():
            low = n_col - 1 - last
            if low == 0:
                msg[1, h, pl.ds(q, 1), :] = degrees()
            part = jnp.zeros((1, width), jnp.float32)
            for s in range(0, last + 1, 4):
                span = slice(s * stride, min(s + 4, last + 1) * stride)
                paths = jnp.dot(y[:, span], x[span, :], preferred_element_type=jnp.float32)
                part += jnp.sum(paths * mask[...], axis=0, keepdims=True)
            msg[low + 1 if low else 0, h, pl.ds(q, 1), :] = part

    me = c * n_row + r

    @pl.when(r != lead)
    def _():
        pl.semaphore_wait(go, 1)

    def post(planes, to):
        mine = msg.at[planes, h, pl.ds(q, 1), :]
        return pltpu.make_async_remote_copy(
            mine, mine, m_send, m_recv, device_id=(lax.rem(to, n_row), to // n_row), device_id_type=MESH)

    others = [i + (i >= me).astype(jnp.int32) for i in range(n_all - 1)]

    @pl.when(c == 0)
    def _():
        for to in others:
            post(pl.ds(0, 2), to).start()

    @pl.when(c > 0)
    def _():
        for to in others:
            post(pl.ds(c + 1, 1), to).start()

    for to in range(n_col - 1):
        @pl.when(to < c)
        def _():
            for e in range(2):
                x_copy(c, e, to).wait_send()

    @pl.when(sends_y)
    def _():
        for o in range(1, n_col):
            y_copy(q, o).wait_send()
    swap.wait_send()

    def take(rows, sem):
        pltpu.make_async_copy(bulk.at[pl.ds(0, rows)], bulk.at[pl.ds(0, rows)], sem).wait()
    pl.when(c == 0)(lambda: take(n_all - 1 + n_row - 1, m_recv))
    pl.when(c > 0)(lambda: take(n_all - 1 + n_row, m_recv))

    closed = sum(msg[p, e] for p in range(n_col + 1) if p != 1 for e in range(2))
    degree = msg[1, 0] + msg[1, 1]
    wedges = jnp.maximum(degree * (degree - 1.0), 1.0)
    ratio = closed / wedges
    wedges = jnp.where(lax.broadcasted_iota(jnp.int32, wedges.shape, 0) < n_col, wedges, 0.0)

    def whole(part):
        return jnp.sum(jnp.sum(part, axis=0, keepdims=True), axis=1, keepdims=True)
    total = whole(closed) / whole(wedges)
    total_ref[0, 0] = total[0, 0]
    for m in range(0, n_mine, 128):
        chunk, lane = spot[0, :, m : m + 128], spot[1, :, m : m + 128]
        found = jnp.zeros((n_sub, 128), jnp.float32)
        for f in range(width // 128):
            picked = jnp.take_along_axis(ratio[:, f * 128 : (f + 1) * 128], lane, axis=1)
            found += jnp.where(chunk == f, picked, 0.0)
        end = min(m + 128, n_mine)
        out_ref[:, m:end] = jnp.sum(found, axis=0, keepdims=True)[:, : end - m]
    pl.when(c == 0)(lambda: take(2 * (n_all - 1), m_send))
    pl.when(c > 0)(lambda: take(n_all - 1, m_send))


def finish(found_ref, total_ref, out_ref, out_total_ref, sems):
    one = pltpu.make_async_copy(found_ref, out_ref, sems.at[0])
    two = pltpu.make_async_copy(total_ref, out_total_ref, sems.at[1])
    one.start()
    two.start()
    one.wait()
    two.wait()


def solution(mesh):
    n_row, n_col = mesh.shape["row"], mesh.shape["col"]
    n_all = n_row * n_col

    def body(adjacency, relabel):
        n_rows, n_words = adjacency.shape
        n_mine = relabel.shape[0]
        depth = 32 * n_words
        width = 2 * n_rows
        lines = n_rows * n_words // 256
        stride = (n_rows + 127) // 128 * 128
        n_sub = max(8, n_col)
        found, total = pl.pallas_call(
            functools.partial(kernel, n_row, n_col),
            out_shape=(pltpu.VMEM((1, n_mine), jnp.float32), pltpu.SMEM((1, 1), jnp.float32)),
            in_specs=[pl.BlockSpec(memory_space=pl.ANY)] * 2,
            out_specs=[pl.BlockSpec(memory_space=pltpu.VMEM), pl.BlockSpec(memory_space=pltpu.SMEM)],
            scratch_shapes=[
                pltpu.VMEM((n_words, n_rows), jnp.int32),
                pltpu.VMEM((2, 2, lines, 1, 128), jnp.int32),
                pltpu.VMEM((n_col, 2, lines, 1, 128), jnp.int32),
                pltpu.VMEM((n_col, 2, lines, 1, 128), jnp.int32),
                pltpu.VMEM((n_col * stride, width), TYPE),
                pltpu.VMEM((depth, n_col * stride), TYPE),
                pltpu.VMEM((depth, width), TYPE),
                pltpu.VMEM((depth, width), jnp.float32),
                pltpu.VMEM((2, n_sub, n_mine + -n_mine % 128), jnp.int32),
                pltpu.VMEM((1, n_mine), jnp.int32),
                pltpu.VMEM((n_col + 1, 2, n_sub, width), jnp.float32),
                pltpu.VMEM((2 * n_all, 1, width), jnp.float32),
                pltpu.SemaphoreType.DMA,
                pltpu.SemaphoreType.DMA,
                pltpu.SemaphoreType.DMA((n_col, 2)),
                pltpu.SemaphoreType.DMA((n_col, 2)),
                pltpu.SemaphoreType.DMA((n_col,)),
                pltpu.SemaphoreType.DMA((n_col,)),
                pltpu.SemaphoreType.DMA,
                pltpu.SemaphoreType.DMA,
                pltpu.SemaphoreType.REGULAR,
                pltpu.SemaphoreType.REGULAR,
                pltpu.SemaphoreType.REGULAR,
                pltpu.SemaphoreType.DMA((2,)),
            ],
            compiler_params=pltpu.CompilerParams(
                collective_id=0, has_side_effects=True, vmem_limit_bytes=60000 * 1024
            ),
        )(adjacency.T, relabel.reshape(1, n_mine))
        clustering, ratio = pl.pallas_call(
            finish,
            out_shape=(
                jax.ShapeDtypeStruct((1, n_mine), jnp.float32),
                jax.ShapeDtypeStruct((1, 1), jnp.float32),
            ),
            in_specs=[pl.BlockSpec(memory_space=pltpu.VMEM), pl.BlockSpec(memory_space=pltpu.SMEM)],
            out_specs=[pl.BlockSpec(memory_space=pl.ANY)] * 2,
            scratch_shapes=[pltpu.SemaphoreType.DMA((2,))],
        )(
            pltpu.with_memory_space_constraint(found, pltpu.VMEM),
            pltpu.with_memory_space_constraint(total, pltpu.SMEM),
        )
        return clustering.reshape(n_mine), ratio.reshape(())

    placed = (P("row", "col"), P(("row", "col")))
    return jax.shard_map(
        body, mesh=mesh, in_specs=placed, out_specs=(P(("row", "col")), P()), check_vma=False
    )
```

```python
import functools

import jax
import jax.numpy as jnp
from jax import lax
from jax.experimental import pallas as pl
from jax.experimental.pallas import tpu as pltpu
from jax.sharding import PartitionSpec as P

MESH = pl.DeviceIdType.MESH
TYPE = jnp.float8_e4m3fn


def unpack(row, times=1):
    wide = jnp.broadcast_to(row, (32, row.shape[1]))
    bits = lax.shift_right_logical(wide, lax.broadcasted_iota(jnp.int32, wide.shape, 0)) & 1
    return (bits * times).astype(jnp.int8).astype(TYPE)


def kernel(
    n_row, n_col, words_ref, relabel_ref, out_ref, total_ref,
    raw, both, px, py, x, y, own, mask, spot, rel, msg, bulk,
    b_send, b_recv, x_send, x_recv, y_send, y_recv, m_send, m_recv, here, ready, go, local_sem,
):
    n_words, n_rows = words_ref.shape
    n_mine = relabel_ref.shape[1]
    spare = -n_mine % 128
    n_all = n_row * n_col
    assert n_row == 2 * n_col and n_words % 4 == 0 and n_rows % 64 == 0
    depth = 32 * n_words
    nw = n_words // 2
    full, half = n_rows // 128, n_rows % 128
    packed = full * nw
    stride = y.shape[1] // n_col
    width, n_sub = msg.shape[3], msg.shape[2]
    r, c = lax.axis_index("row"), lax.axis_index("col")
    q, h = r // 2, lax.rem(r, 2)
    pair = r + 1 - 2 * h
    barrier = pltpu.get_barrier_semaphore()
    load = pltpu.make_async_copy(words_ref, raw, local_sem.at[0])
    load_r = pltpu.make_async_copy(relabel_ref, rel, local_sem.at[1])
    load.start()
    load_r.start()
    lead = 1
    sends_y = q >= c
    for o in range(1, n_row):
        p = lax.rem(r + o, n_row)

        @pl.when((p == pair) | ((lax.rem(p, 2) == h) & (p // 2 >= c)) | (r == lead))
        def _():
            pl.semaphore_signal(barrier, inc=1, device_id=(p, c), device_id_type=MESH)

    def greet_above():
        for k in range(1, n_col):
            @pl.when(k > c)
            def _():
                for e in range(2):
                    pl.semaphore_signal(barrier, inc=1, device_id=(2 * q + e, k), device_id_type=MESH)
    greet_above()
    load.wait()
    for e in range(2):
        for w in range(nw):
            for f in range(full):
                both[h, e, f * nw + w] = raw[e * nw + w : e * nw + w + 1, f * 128 : (f + 1) * 128]
        if half:
            for t in range(nw // 2):
                two = [raw[e * nw + t + d : e * nw + t + d + 1, full * 128 :] for d in (0, nw // 2)]
                both[h, e, packed + t] = jnp.concatenate(two, axis=1)
    known = (r == lead) | (pair == lead) | (sends_y & (h == lead % 2))
    pl.semaphore_wait(barrier, 2 * c + jnp.where(sends_y, n_col, 1) + jnp.where(known, 0, 1))

    def x_copy(k, e, to):
        return pltpu.make_async_remote_copy(
            both.at[h, e], px.at[k, h], x_send.at[to, e], x_recv.at[k, h],
            device_id=(2 * q + e, to), device_id_type=MESH)

    def y_copy(k, o):
        to = 2 * lax.rem(q + o, n_col) + h
        return pltpu.make_async_remote_copy(
            both.at[h], py.at[k], y_send.at[o], y_recv.at[k], device_id=(to, c), device_id_type=MESH)

    swap = pltpu.make_async_remote_copy(
        both.at[h], both.at[h], b_send, b_recv, device_id=(pair, c), device_id_type=MESH)

    for to in range(n_col - 1):
        @pl.when(to < c)
        def _():
            for e in range(2):
                x_copy(c, e, to).start()

    @pl.when(sends_y)
    def _():
        for o in range(n_col - 1, 0, -1):
            y_copy(q, o).start()
    swap.start()

    @pl.when(r != lead)
    def _():
        pl.semaphore_signal(here, inc=1, device_id=(lead, c), device_id_type=MESH)

    py[q] = both[h]
    if n_sub > n_col:
        for p in range(n_col + 1):
            for e in range(2):
                msg[p, e, n_col:, :] = jnp.zeros((n_sub - n_col, width), jnp.float32)
    if half:
        for k in range(n_col):
            x[k * stride + n_rows : (k + 1) * stride, :] = jnp.zeros((stride - n_rows, width), TYPE)
    load_r.wait()
    label = rel[...]
    if spare:
        label = jnp.concatenate([label, jnp.zeros((1, spare), jnp.int32)], axis=1)
    label = jnp.broadcast_to(label, (n_sub, n_mine + spare))
    owner = jnp.zeros_like(label)
    for k in range(1, n_row):
        owner += (label >= k * n_rows).astype(jnp.int32)
    place = label - owner * n_rows
    part = owner & 1
    lane = jnp.where(
        place < full * 128, part * (full * 128) + place, full * 128 + part * 64 + place)
    mine = lax.shift_right_logical(owner, 1) == lax.broadcasted_iota(jnp.int32, owner.shape, 0)
    spot[0] = jnp.where(mine, lax.shift_right_logical(lane, 7), -1)
    spot[1] = lane & 127

    above = n_col - 1 - c

    def slot(k):
        return k - c

    left = lax.broadcasted_iota(jnp.int32, (1, 128), 1) < 64

    def spread(a, b, into, start, times):
        ends = [None] * nw
        if half:
            for t in range(nw // 2):
                one, two = a(packed + t), b(packed + t)
                ends[t] = jnp.where(left, one, pltpu.roll(two, 64, 1))
                ends[t + nw // 2] = jnp.where(left, pltpu.roll(one, 64, 1), two)
        for w in range(nw):
            rows = pl.ds(pl.multiple_of(start + w * 32, 32), 32)
            for e, get in enumerate((a, b)):
                for f in range(full):
                    at = (e * full + f) * 128
                    into[rows, at : at + 128] = unpack(get(f * nw + w), times)
            if half:
                into[rows, 2 * full * 128 :] = unpack(ends[w], times)

    def take_x(k):
        for e in range(2):
            pltpu.make_async_remote_copy(
                px.at[k, e], px.at[k, e], x_send.at[0, 0], x_recv.at[k, e],
                device_id=(r, 0), device_id_type=MESH).wait_recv()
        spread(lambda i: px[k, 0, i], lambda i: px[k, 1, i], x, slot(k) * stride, 2)

    def take_y(k):
        @pl.when(k != q)
        def _():
            pltpu.make_async_remote_copy(
                py.at[k], py.at[k], y_send.at[0], y_recv.at[k], device_id=(r, c), device_id_type=MESH).wait_recv()

        def lanes(f):
            return pl.ds(pl.multiple_of(slot(k) * stride + f * 128, 128), 128)
        for e in range(2):
            for w in range(nw):
                rows = slice((e * nw + w) * 32, (e * nw + w + 1) * 32)
                for f in range(full):
                    y[rows, lanes(f)] = unpack(py[k, e, f * nw + w])
                if half:
                    ends = py[k, e, packed + w % (nw // 2)]
                    y[rows, lanes(full)] = unpack(ends if w < nw // 2 else pltpu.roll(ends, 64, 1))

    def hear():
        pl.semaphore_wait(here, n_row - 1)
        for k in range(n_col - 1):
            @pl.when(k < c)
            def _():
                pl.semaphore_signal(ready, inc=1, device_id=(r, k), device_id_type=MESH)
        pl.when(c == n_col - 1)(tell)

    def tell():
        @pl.when(c < n_col - 1)
        def _():
            pl.semaphore_wait(ready, n_col - 1 - c)
        for o in range(1, n_row):
            pl.semaphore_signal(go, inc=1, device_id=(lax.rem(r + o, n_row), c), device_id_type=MESH)

    swap.wait_recv()
    for e in range(2):
        spread(lambda i: both[0, e, i], lambda i: both[1, e, i], own, e * n_rows, 1)
    mask[...] = own[...].astype(jnp.float32)
    x[0:n_rows, :] = own[pl.ds(pl.multiple_of(h * n_rows, 32), n_rows), :]

    def next_y(j, carry):
        k = jnp.where(j == 0, q, n_col - j - (q >= n_col - j).astype(jnp.int32))
        pl.when(k >= c)(lambda: take_y(k))
        return carry
    pl.when(r == lead)(hear)
    lax.fori_loop(0, n_col, next_y, 0)

    def next_x(j, carry):
        pl.when((j == above) & (r == lead))(tell)
        take_x(c + j)
        return carry

    def degrees():
        sums = []
        for e in range(2):
            count = lax.population_count(both[e, h])
            for k in range(1, n_col):
                count += lax.population_count(px[k, e])
            sums.append([jnp.sum(count[f * nw : (f + 1) * nw], axis=0) for f in range(full)])
            if half:
                ends = jnp.sum(count[packed:], axis=0)
                sums[e].append(ends + pltpu.roll(ends, 64, 1))
        lines = sums[0][:full] + sums[1][:full]
        if half:
            lines.append(jnp.where(left, sums[0][full], sums[1][full]))
        return jnp.concatenate(lines, axis=1).astype(jnp.float32)

    for last in range(n_col):
        @pl.when(above == last)
        def _():
            low = n_col - 1 - last

            def add(start, end):
                part = jnp.zeros((1, width), jnp.float32)
                for s in range(start, end, 4):
                    span = slice(s * stride, min(s + 4, end) * stride)
                    paths = jnp.dot(y[:, span], x[span, :], preferred_element_type=jnp.float32)
                    part += jnp.sum(paths * mask[...], axis=0, keepdims=True)
                return part
            early = last if last > 1 else last + 1
            lax.fori_loop(1, early, next_x, 0)
            part = add(0, early)
            if early == last:
                row = msg.at[low + 1 if low else 0, h, pl.ds(q, 1), :]
                row[...] = part
                next_x(last, 0)
                part = row[...] + add(last, last + 1)
            if low == 0:
                msg[1, h, pl.ds(q, 1), :] = degrees()
            msg[low + 1 if low else 0, h, pl.ds(q, 1), :] = part

    me = c * n_row + r

    @pl.when(r != lead)
    def _():
        pl.semaphore_wait(go, 1)

    def post(planes, to):
        mine = msg.at[planes, h, pl.ds(q, 1), :]
        return pltpu.make_async_remote_copy(
            mine, mine, m_send, m_recv, device_id=(lax.rem(to, n_row), to // n_row), device_id_type=MESH)

    others = [i + (i >= me).astype(jnp.int32) for i in range(n_all - 1)]

    @pl.when(c == 0)
    def _():
        for to in others:
            post(pl.ds(0, 2), to).start()

    @pl.when(c > 0)
    def _():
        for to in others:
            post(pl.ds(c + 1, 1), to).start()

    for to in range(n_col - 1):
        @pl.when(to < c)
        def _():
            for e in range(2):
                x_copy(c, e, to).wait_send()

    @pl.when(sends_y)
    def _():
        for o in range(1, n_col):
            y_copy(q, o).wait_send()
    swap.wait_send()

    def take(rows, sem):
        pltpu.make_async_copy(bulk.at[pl.ds(0, rows)], bulk.at[pl.ds(0, rows)], sem).wait()
    pl.when(c == 0)(lambda: take(n_all - 1 + n_row - 1, m_recv))
    pl.when(c > 0)(lambda: take(n_all - 1 + n_row, m_recv))

    closed = sum(msg[p, e] for p in range(n_col + 1) if p != 1 for e in range(2))
    degree = msg[1, 0] + msg[1, 1]
    wedges = jnp.maximum(degree * (degree - 1.0), 1.0)
    ratio = closed / wedges
    wedges = jnp.where(lax.broadcasted_iota(jnp.int32, wedges.shape, 0) < n_col, wedges, 0.0)

    def whole(part):
        return jnp.sum(jnp.sum(part, axis=0, keepdims=True), axis=1, keepdims=True)
    total = whole(closed) / whole(wedges)
    total_ref[0, 0] = total[0, 0]
    for m in range(0, n_mine, 128):
        chunk, lane = spot[0, :, m : m + 128], spot[1, :, m : m + 128]
        found = jnp.zeros((n_sub, 128), jnp.float32)
        for f in range(width // 128):
            picked = jnp.take_along_axis(ratio[:, f * 128 : (f + 1) * 128], lane, axis=1)
            found += jnp.where(chunk == f, picked, 0.0)
        end = min(m + 128, n_mine)
        out_ref[:, m:end] = jnp.sum(found, axis=0, keepdims=True)[:, : end - m]
    pl.when(c == 0)(lambda: take(2 * (n_all - 1), m_send))
    pl.when(c > 0)(lambda: take(n_all - 1, m_send))


def finish(found_ref, total_ref, out_ref, out_total_ref, sems):
    one = pltpu.make_async_copy(found_ref, out_ref, sems.at[0])
    two = pltpu.make_async_copy(total_ref, out_total_ref, sems.at[1])
    one.start()
    two.start()
    one.wait()
    two.wait()


def solution(mesh):
    n_row, n_col = mesh.shape["row"], mesh.shape["col"]
    n_all = n_row * n_col

    def body(adjacency, relabel):
        n_rows, n_words = adjacency.shape
        n_mine = relabel.shape[0]
        depth = 32 * n_words
        width = 2 * n_rows
        lines = n_rows * n_words // 256
        stride = (n_rows + 127) // 128 * 128
        n_sub = max(8, n_col)
        found, total = pl.pallas_call(
            functools.partial(kernel, n_row, n_col),
            out_shape=(pltpu.VMEM((1, n_mine), jnp.float32), pltpu.SMEM((1, 1), jnp.float32)),
            in_specs=[pl.BlockSpec(memory_space=pl.ANY)] * 2,
            out_specs=[pl.BlockSpec(memory_space=pltpu.VMEM), pl.BlockSpec(memory_space=pltpu.SMEM)],
            scratch_shapes=[
                pltpu.VMEM((n_words, n_rows), jnp.int32),
                pltpu.VMEM((2, 2, lines, 1, 128), jnp.int32),
                pltpu.VMEM((n_col, 2, lines, 1, 128), jnp.int32),
                pltpu.VMEM((n_col, 2, lines, 1, 128), jnp.int32),
                pltpu.VMEM((n_col * stride, width), TYPE),
                pltpu.VMEM((depth, n_col * stride), TYPE),
                pltpu.VMEM((depth, width), TYPE),
                pltpu.VMEM((depth, width), jnp.float32),
                pltpu.VMEM((2, n_sub, n_mine + -n_mine % 128), jnp.int32),
                pltpu.VMEM((1, n_mine), jnp.int32),
                pltpu.VMEM((n_col + 1, 2, n_sub, width), jnp.float32),
                pltpu.VMEM((2 * n_all, 1, width), jnp.float32),
                pltpu.SemaphoreType.DMA,
                pltpu.SemaphoreType.DMA,
                pltpu.SemaphoreType.DMA((n_col, 2)),
                pltpu.SemaphoreType.DMA((n_col, 2)),
                pltpu.SemaphoreType.DMA((n_col,)),
                pltpu.SemaphoreType.DMA((n_col,)),
                pltpu.SemaphoreType.DMA,
                pltpu.SemaphoreType.DMA,
                pltpu.SemaphoreType.REGULAR,
                pltpu.SemaphoreType.REGULAR,
                pltpu.SemaphoreType.REGULAR,
                pltpu.SemaphoreType.DMA((2,)),
            ],
            compiler_params=pltpu.CompilerParams(
                collective_id=0, has_side_effects=True, vmem_limit_bytes=60000 * 1024
            ),
        )(adjacency.T, relabel.reshape(1, n_mine))
        clustering, ratio = pl.pallas_call(
            finish,
            out_shape=(
                jax.ShapeDtypeStruct((1, n_mine), jnp.float32),
                jax.ShapeDtypeStruct((1, 1), jnp.float32),
            ),
            in_specs=[pl.BlockSpec(memory_space=pltpu.VMEM), pl.BlockSpec(memory_space=pltpu.SMEM)],
            out_specs=[pl.BlockSpec(memory_space=pl.ANY)] * 2,
            scratch_shapes=[pltpu.SemaphoreType.DMA((2,))],
        )(
            pltpu.with_memory_space_constraint(found, pltpu.VMEM),
            pltpu.with_memory_space_constraint(total, pltpu.SMEM),
        )
        return clustering.reshape(n_mine), ratio.reshape(())

    placed = (P("row", "col"), P(("row", "col")))
    return jax.shard_map(
        body, mesh=mesh, in_specs=placed, out_specs=(P(("row", "col")), P()), check_vma=False
    )
```
